256 devices in a mesh: tm: 4 (over x), rows: 64 (over z, y, core).
Axes of the slice: x: 4, y: 4, z: 8, core: 2. Of those that a mesh axis runs over, the one named last changes fastest.
Arguments:
- latents: bfloat16 [8, 128, 256, 256], P('tm', 'rows'), may hold values from -40 to 40
- norm1_gain: float32 [256], replicated, may hold values from 0.25 to 1.75
- norm1_shift: float32 [256], replicated, may hold values from -3 to 3
- conv1_weight: bfloat16 [3, 3, 3, 256, 256], replicated, may hold values from -0.078125 to 0.078125
- conv1_bias: float32 [256], replicated, may hold values from -3 to 3
- norm2_gain: float32 [256], replicated, may hold values from 0.25 to 1.75
- norm2_shift: float32 [256], replicated, may hold values from -3 to 3
- conv2_weight: bfloat16 [3, 3, 3, 256, 256], replicated, may hold values from -0.078125 to 0.078125
- conv2_bias: float32 [256], replicated, may hold values from -3 to 3
- up_weight: bfloat16 [256, 2048], replicated, may hold values from -0.375 to 0.375
- up_bias: float32 [2048], replicated, may hold values from -3 to 3
Outputs:
- video: bfloat16 [16, 256, 512, 256], P('tm', 'rows')
The draws below stay inside these ranges and needn't reach their ends.
All inputs are finite; a program needn't handle non-finite values.
Results may differ from the reference program's by a relative error of at most 0.0051.
Values may be sent and summed in bfloat16 or wider, within the bound.
No kernel may reach another device: no remote copies, remote signals or barrier semaphores. Data moves between devices by JAX's collectives and lax.ppermute only.
A program may use at most 64 MiB of HBM per device.

```python
import jax
import jax.numpy as jnp
from jax import lax

C = 256
GROUPS = 32
W = 256
NF = 8
NR = 128


def draw_latents(key, part):
    first, second, third, fourth, fifth, sixth = jax.random.split(jax.random.fold_in(key, 11), 6)
    frame_pos = jnp.arange(NF, dtype=jnp.float32) / max(NF - 1, 1)
    row_pos = jnp.arange(NR, dtype=jnp.float32) / max(NR - 1, 1)
    column_pos = jnp.arange(W, dtype=jnp.float32) / W
    frame_rough = 2.0 ** jax.random.uniform(fourth, (NF,), jnp.float32, -0.5, 0.5)
    row_rough = 2.0 ** jax.random.uniform(fifth, (NR,), jnp.float32, -0.5, 0.5)
    phase = jax.random.uniform(sixth, (), jnp.float32, 0.0, 2.0 * jnp.pi)
    column_profile = 2.0 ** (0.6 * jnp.sin(2.0 * jnp.pi * column_pos + phase))
    frame_factor = 3.0 ** frame_pos * frame_rough
    row_factor = 3.0 ** row_pos * row_rough
    spatial = frame_factor[:, None] * row_factor[None, :] / 3.0
    rough = jax.random.uniform(third, (NF, NR, W, 1), jnp.float32, 0.5, 1.5)
    noise = jnp.clip(jax.random.normal(first, (NF, NR, W, C), jnp.float32), -4.0, 4.0)
    channel_scale = 2.0 ** jax.random.uniform(second, (C,), jnp.float32, -1.0, 1.0)
    offset_val = 0.3
    values = spatial[:, :, None, None] * column_profile[None, None, :, None] * rough * channel_scale * (offset_val + noise)
    values = jnp.clip(values, -40.0, 40.0)
    return values.astype(jnp.bfloat16)


def gaussian(key, dims, scale, bound, kind=jnp.bfloat16):
    result = jax.random.normal(key, dims, jnp.float32) * scale
    return jnp.minimum(jnp.maximum(result, -bound), bound).astype(kind)


def setup_inputs(seed: int = 0) -> dict:
    key_of = jax.random.split(jax.random.key(seed), 12)
    latents = draw_latents(jax.random.fold_in(key_of[11], 71), 0)
    norm1_gain = jnp.clip(1.0 + 0.15 * jax.random.normal(key_of[1], (C,), jnp.float32), 0.25, 1.75)
    norm1_shift = gaussian(key_of[2], (C,), 0.5, 3.0, jnp.float32)
    conv1_weight = gaussian(key_of[3], (3, 3, 3, C, C), (27 * C) ** -0.5, 0.078125)
    conv1_bias = gaussian(key_of[4], (C,), 0.5, 3.0, jnp.float32)
    norm2_gain = jnp.clip(1.0 + 0.15 * jax.random.normal(key_of[5], (C,), jnp.float32), 0.25, 1.75)
    norm2_shift = gaussian(key_of[6], (C,), 0.5, 3.0, jnp.float32)
    conv2_weight = gaussian(key_of[7], (3, 3, 3, C, C), (27 * C) ** -0.5, 0.078125)
    conv2_bias = gaussian(key_of[8], (C,), 0.5, 3.0, jnp.float32)
    up_weight = gaussian(key_of[9], (C, 8 * C), C ** -0.5, 0.375)
    up_bias = gaussian(key_of[10], (8 * C,), 0.5, 3.0, jnp.float32)
    return dict(latents=latents, norm1_gain=norm1_gain, norm1_shift=norm1_shift, conv1_weight=conv1_weight, conv1_bias=conv1_bias, norm2_gain=norm2_gain, norm2_shift=norm2_shift, conv2_weight=conv2_weight, conv2_bias=conv2_bias, up_weight=up_weight, up_bias=up_bias)


EPSILON = 1e-06

def normed_act(values, gain_vec, shift_vec):
    grouped = values.reshape(-1, GROUPS, C // GROUPS)
    group_mean = lax.optimization_barrier(jnp.mean(grouped, axis=(0, 2)))
    centred = grouped - group_mean[None, :, None]
    variance = lax.optimization_barrier(jnp.mean(centred * centred, axis=(0, 2)))
    scaled = (centred / jnp.sqrt(variance + EPSILON)[None, :, None]).reshape(values.shape)
    return jax.nn.silu(scaled * gain_vec + shift_vec).astype(jnp.bfloat16)

def causal_conv(act, weight, bias_vec):
    padded = jnp.pad(act, ((2, 0), (1, 1), (1, 1), (0, 0)))
    summed = jnp.zeros((NF * NR * W, C), jnp.float32)
    for i in range(3):
        for j in range(3):
            for k in range(3):
                window = padded[i:i + NF, j:j + NR, k:k + W].reshape(-1, C)
                summed = summed + jnp.dot(window, weight[i, j, k], preferred_element_type=jnp.float32)
    return summed.reshape(NF, NR, W, C) + bias_vec

def reference(latents, norm1_gain, norm1_shift, conv1_weight, conv1_bias, norm2_gain, norm2_shift, conv2_weight, conv2_bias, up_weight, up_bias):
    latent_f32 = latents.astype(jnp.float32)
    act_one = normed_act(latent_f32, norm1_gain, norm1_shift)
    hidden = causal_conv(act_one, conv1_weight, conv1_bias)
    act_two = normed_act(hidden, norm2_gain, norm2_shift)
    block_out = (latent_f32 + causal_conv(act_two, conv2_weight, conv2_bias)).astype(jnp.bfloat16)
    widened = (jnp.dot(block_out.reshape(-1, C), up_weight, preferred_element_type=jnp.float32) + up_bias).astype(jnp.bfloat16)
    widened = widened.reshape(NF, NR, W, 2, 2, 2, C).transpose(0, 3, 1, 4, 2, 5, 6)
    return widened.reshape(2 * NF, 2 * NR, 2 * W, C)
```

```python
import functools

import jax
import jax.numpy as jnp
from jax import lax
from jax.experimental import pallas as pl
from jax.experimental.pallas import tpu as pltpu
from jax.sharding import Mesh
from jax.sharding import PartitionSpec as P

GROUPS = 32
EPSILON = 1e-06
ROWS = ("rows_0", "rows_1", "rows_2")
EVERY = ("tm", "rows_0", "rows_1", "rows_2")
EXACT = lax.Precision.HIGHEST
F32 = jnp.float32
BF16 = jnp.bfloat16
LANES = 128


def exact_dot(a, b):
    return jnp.dot(a, b, precision=EXACT, preferred_element_type=F32)


def group_of_channel(channels, lane_base):
    per_group = channels // GROUPS
    lane = lax.broadcasted_iota(jnp.int32, (LANES, channels), 0)
    group = lax.broadcasted_iota(jnp.int32, (LANES, channels), 1) // per_group
    return (lane == group + lane_base).astype(F32)


def channel_to_group(channels, lane_base):
    per_group = channels // GROUPS
    group = lax.broadcasted_iota(jnp.int32, (channels, LANES), 0) // per_group
    lane = lax.broadcasted_iota(jnp.int32, (channels, LANES), 1)
    return (lane == group + lane_base).astype(F32)


def pack_moments(channel_sum, channel_square, count):
    channels = channel_sum.shape[1]
    per_group = channels // GROUPS
    channel_mean = channel_sum * (1.0 / count)
    group_mean = exact_dot(channel_mean, channel_to_group(channels, 0)) * (1.0 / per_group)
    spread = channel_mean - exact_dot(group_mean, group_of_channel(channels, 0))
    return group_mean + exact_dot(
        channel_square + spread * spread * count, channel_to_group(channels, GROUPS)
    )


def merge_moments(gathered, count, gain, shift, channels):
    devices = gathered.shape[0]
    total = jnp.broadcast_to(jnp.sum(gathered, axis=0, keepdims=True), (8, LANES))
    mean = total * (1.0 / devices)
    away = gathered - mean[0:1]
    between = jnp.broadcast_to(jnp.sum(away * away, axis=0, keepdims=True), (8, LANES))
    by_group = group_of_channel(channels, 0)
    mean_c = exact_dot(mean, by_group)
    within_c = exact_dot(total, group_of_channel(channels, GROUPS))
    between_c = exact_dot(between, by_group) * count
    variance = (within_c + between_c) * (1.0 / (count * devices))
    scale = gain / jnp.sqrt(variance + EPSILON)
    return 0.5 * scale, 0.5 * (shift - mean_c * scale)


def stats_kernel(values_ref, out_ref, *, devices):
    channels = values_ref.shape[-1]
    blocks = values_ref.shape[0] * values_ref.shape[1]
    width = values_ref.shape[2]
    flat = values_ref.reshape(blocks, width, channels)
    count = blocks * width

    def add(i, acc):
        return acc + jnp.sum(flat[i].astype(F32).reshape(width // 8, 8, channels), axis=0)

    zero = jnp.zeros((8, channels), F32)
    acc = lax.fori_loop(0, blocks, add, zero)
    channel_sum = jnp.broadcast_to(jnp.sum(acc, axis=0, keepdims=True), (8, channels))
    mean = channel_sum * (1.0 / count)

    def add_square(i, acc):
        away = flat[i].astype(F32).reshape(width // 8, 8, channels) - mean[None]
        return acc + jnp.sum(away * away, axis=0)

    acc = lax.fori_loop(0, blocks, add_square, zero)
    channel_square = jnp.broadcast_to(jnp.sum(acc, axis=0, keepdims=True), (8, channels))
    packed = pack_moments(channel_sum, channel_square, count)
    out_ref[...] = jnp.broadcast_to(packed[0:1], (devices, LANES))


def fill_acts(act_ref, own_ref, prior_ref, inter_ref, intra_ref, place_ref, scale, offset, bias):
    width, channels = own_ref.shape[2], own_ref.shape[3]
    piece = 64

    def act(block, keep):
        def step(p, _):
            for s in range(2):
                at = pl.ds(pl.multiple_of((p * 2 + s) * (piece // 2), piece // 2), piece // 2)
                yield_at = at
                source, target = block
                v = source[yield_at].astype(F32)
                if bias is not None:
                    v = v + bias[0:1]
                h = v * scale[0:1] + offset[0:1]
                target[yield_at] = ((h + h * jnp.tanh(h)) * keep).astype(BF16)
            return 0

        lax.fori_loop(0, width // piece, step, 0)

    core = place_ref[0]
    frame_keep = place_ref[1].astype(F32)
    inter_keep = place_ref[2].astype(F32)
    inter_row = core * 3
    for f in range(4):
        keep = frame_keep if f < 2 else jnp.float32(1.0)
        source = prior_ref.at[f] if f < 2 else own_ref.at[f - 2]
        for r in range(2):
            act((source.at[r], act_ref.at[f, r + 1]), keep)
        act((inter_ref.at[f], act_ref.at[f, inter_row]), keep * inter_keep)
        act((intra_ref.at[f], act_ref.at[f, 3 - inter_row]), keep)


def conv_frame(act_ref, weight_ref, t):
    width, channels = act_ref.shape[2], act_ref.shape[3]
    q = lax.broadcasted_iota(jnp.int32, (2 * width, channels), 0) % width
    total = None
    for k in (1, 0, 2):
        acc = None
        for i in range(3):
            for j in range(3):
                window = act_ref[t + i, j : j + 2].reshape(2 * width, channels)
                part = jnp.dot(window, weight_ref[i, j, k], preferred_element_type=F32)
                acc = part if acc is None else acc + part
        if k == 0:
            acc = jnp.where(q == 0, 0.0, pltpu.roll(acc, 1, 0))
        elif k == 2:
            acc = jnp.where(q == width - 1, 0.0, pltpu.roll(acc, 2 * width - 1, 0))
        total = acc if total is None else total + acc
    return total


def first_kernel(
    place_ref, own_ref, prior_ref, inter_ref, intra_ref, gathered_ref, gain_ref, shift_ref, bias_ref, weight_ref,
    hidden_ref, moments_ref, act_ref, sum_ref,
):
    t = pl.program_id(0)
    width, channels = own_ref.shape[2], own_ref.shape[3]
    devices = gathered_ref.shape[0]
    per_device = 4 * width * (channels // GROUPS)

    @pl.when(t == 0)
    def _():
        gain = jnp.broadcast_to(gain_ref[...], (8, channels))
        shift = jnp.broadcast_to(shift_ref[...], (8, channels))
        scale, offset = merge_moments(gathered_ref[...], per_device, gain, shift, channels)
        fill_acts(act_ref, own_ref, prior_ref, inter_ref, intra_ref, place_ref, scale, offset, None)

    hidden = conv_frame(act_ref, weight_ref, t)
    hidden_ref[0] = hidden.reshape(2, width, channels).astype(BF16)
    folded = hidden.reshape(2 * width // 8, 8, channels)
    count = 2.0 * width
    frame_sum = jnp.broadcast_to(jnp.sum(jnp.sum(folded, axis=0), axis=0, keepdims=True), (8, channels))
    frame_mean = frame_sum * (1.0 / count)
    away = folded - frame_mean[None]
    frame_square = jnp.broadcast_to(jnp.sum(jnp.sum(away * away, axis=0), axis=0, keepdims=True), (8, channels))

    @pl.when(t == 0)
    def _():
        sum_ref[0] = frame_sum
        sum_ref[1] = frame_square

    @pl.when(t == 1)
    def _():
        apart = (frame_sum - sum_ref[0]) * (1.0 / count)
        both = frame_sum + sum_ref[0] + (2.0 * count) * bias_ref[...]
        square = frame_square + sum_ref[1] + apart * apart * (0.5 * count)
        packed = pack_moments(both, square, 2.0 * count)
        moments_ref[...] = jnp.broadcast_to(packed[0:1], (devices, LANES))


def second_kernel(
    place_ref, latents_ref, own_ref, prior_ref, inter_ref, intra_ref, gathered_ref, gain_ref, shift_ref, bias1_ref,
    bias2_ref, weight_ref, up_ref, up_bias_ref, video_ref, act_ref, wide_ref,
):
    t = pl.program_id(0)
    width, channels = own_ref.shape[2], own_ref.shape[3]
    per_device = 4 * width * (channels // GROUPS)

    @pl.when(t == 0)
    def _():
        gain = jnp.broadcast_to(gain_ref[...], (8, channels))
        shift = jnp.broadcast_to(shift_ref[...], (8, channels))
        scale, offset = merge_moments(gathered_ref[...], per_device, gain, shift, channels)
        fill_acts(act_ref, own_ref, prior_ref, inter_ref, intra_ref, place_ref, scale, offset, bias1_ref[...])

    conv = conv_frame(act_ref, weight_ref, t) + bias2_ref[...]
    latents = latents_ref[0].reshape(2 * width, channels).astype(F32)
    block_out = (latents + conv).astype(BF16)
    for a in range(2):
        for b in range(2):
            for e in range(2):
                n = ((2 * a + b) * 2 + e) * channels
                part = jnp.dot(block_out, up_ref[:, n : n + channels], preferred_element_type=F32)
                part = part + up_bias_ref[:, n : n + channels]
                for lane in range(0, channels, LANES):
                    wide_ref[lane // LANES, pl.ds(e, 2 * width, stride=2), :] = part[:, lane : lane + LANES]
            for r in range(2):
                for lane in range(0, channels, LANES):
                    video_ref[a, 2 * r + b, :, lane : lane + LANES] = wide_ref[
                        lane // LANES, 2 * width * r : 2 * width * (r + 1), :
                    ].astype(BF16)


def whole(shape, memory_space=None):
    zeros = (0,) * len(shape)
    if memory_space is not None:
        return pl.BlockSpec(memory_space=memory_space)
    return pl.BlockSpec(shape, lambda *_: zeros, pipeline_mode=pl.Buffered(1))


def exchange(cells, core):
    tm = lax.axis_size("tm")
    rows = lax.axis_size(ROWS)
    prior = lax.ppermute(cells, "tm", [(i, i + 1) for i in range(tm - 1)])
    return prior, rows


def edges(cells, prior, core):
    rows = lax.axis_size(ROWS)
    four = jnp.concatenate([prior, cells], axis=0)
    outward = lax.dynamic_index_in_dim(four, core, axis=1, keepdims=False)
    inward = lax.dynamic_index_in_dim(four, 1 - core, axis=1, keepdims=False)
    between = [(i, i + 1) for i in range(1, rows - 1, 2)] + [(i + 1, i) for i in range(1, rows - 1, 2)]
    within = [(i, i ^ 1) for i in range(rows)]
    return lax.ppermute(outward, ROWS, between), lax.ppermute(inward, ROWS, within)


def share(moments, devices):
    return lax.all_to_all(moments, EVERY, split_axis=0, concat_axis=0, tiled=True)


def body(
    latents,
    norm1_gain,
    norm1_shift,
    conv1_weight,
    conv1_bias,
    norm2_gain,
    norm2_shift,
    conv2_weight,
    conv2_bias,
    up_weight,
    up_bias,
):
    frames, rows, width, channels = latents.shape
    devices = lax.axis_size(EVERY)
    core = lax.axis_index("rows_2")
    row_block = lax.axis_index(ROWS)
    edge = jnp.where(core == 0, row_block == 0, row_block == lax.axis_size(ROWS) - 1)
    place = jnp.stack(
        [core, (lax.axis_index("tm") > 0).astype(jnp.int32), 1 - edge.astype(jnp.int32)]
    ).astype(jnp.int32)
    row = lambda v: v.reshape(1, -1)
    limit = pltpu.CompilerParams(dimension_semantics=("arbitrary",), vmem_limit_bytes=56 * 1024 * 1024)

    prior, _ = exchange(latents, core)
    moments = pl.pallas_call(
        functools.partial(stats_kernel, devices=devices),
        out_shape=jax.ShapeDtypeStruct((devices, LANES), F32),
    )(latents)
    gathered = share(moments, devices)
    inter, intra = edges(latents, prior, core)

    smem = whole((3,), pltpu.MemorySpace.SMEM)
    cells = whole((frames, rows, width, channels))
    edge_cells = whole((2 * frames, width, channels))
    vector = whole((1, channels))
    weights = whole((3, 3, 3, channels, channels))
    acts = pltpu.VMEM((2 * frames, rows + 2, width, channels), BF16)
    hidden, moments = pl.pallas_call(
        first_kernel,
        grid=(frames,),
        in_specs=[
            smem, cells, cells, edge_cells, edge_cells, whole((devices, LANES)), vector, vector, vector, weights,
        ],
        out_specs=[
            pl.BlockSpec((1, rows, width, channels), lambda t: (t, 0, 0, 0)),
            whole((devices, LANES)),
        ],
        out_shape=[
            jax.ShapeDtypeStruct(latents.shape, BF16),
            jax.ShapeDtypeStruct((devices, LANES), F32),
        ],
        scratch_shapes=[acts, pltpu.VMEM((2, 8, channels), F32)],
        compiler_params=limit,
    )(
        place, latents, prior, inter, intra, gathered, row(norm1_gain), row(norm1_shift), row(conv1_bias), conv1_weight
    )

    prior, _ = exchange(hidden, core)
    gathered = share(moments, devices)
    inter, intra = edges(hidden, prior, core)
    frame = lambda t: (t, 0, 0, 0)
    return pl.pallas_call(
        second_kernel,
        grid=(frames,),
        in_specs=[
            smem, pl.BlockSpec((1, rows, width, channels), frame), cells, cells, edge_cells, edge_cells,
            whole((devices, LANES)), vector, vector, vector, vector, weights, whole(up_weight.shape),
            whole((1, up_bias.shape[0])),
        ],
        out_specs=pl.BlockSpec((2, 2 * rows, 2 * width, channels), frame),
        out_shape=jax.ShapeDtypeStruct((2 * frames, 2 * rows, 2 * width, channels), BF16),
        scratch_shapes=[acts, pltpu.VMEM((channels // LANES, 2 * rows * width, LANES), F32)],
        compiler_params=limit,
    )(
        place, latents, hidden, prior, inter, intra, gathered, row(norm2_gain), row(norm2_shift), row(conv1_bias),
        row(conv2_bias), conv2_weight, up_weight, row(up_bias),
    )


def solution(mesh):
    finer = Mesh(
        mesh.devices.reshape(mesh.shape["tm"], 8, 4, 2), ("tm", "rows_0", "rows_1", "rows_2")
    )
    placed = (P("tm", ROWS, None, None), P(), P(), P(), P(), P(), P(), P(), P(), P(), P())
    return jax.shard_map(
        body, mesh=finer, in_specs=placed, out_specs=P("tm", ROWS, None, None), check_vma=False
    )
```

```python
import functools

import jax
import jax.numpy as jnp
from jax import lax
from jax.experimental import pallas as pl
from jax.experimental.pallas import tpu as pltpu
from jax.sharding import Mesh
from jax.sharding import PartitionSpec as P


GROUPS = 32
EPSILON = 1e-06
ROWS = ("rows_0", "rows_1", "rows_2")
EVERY = ("tm", "rows_0", "rows_1", "rows_2")
F32 = jnp.float32
BF16 = jnp.bfloat16
LANES = 128


def split_rows(first, second):
    row = lax.broadcasted_iota(jnp.int32, first.shape, 0)
    value = jnp.where(row < 3, first, second)
    high = value.astype(BF16).astype(F32)
    middle = (value - high).astype(BF16).astype(F32)
    low = value - high - middle
    step = jnp.where(row < 3, row, row - 3)
    part = jnp.where(step == 0, high, jnp.where(step == 1, middle, low))
    return jnp.where(row < 6, part, 0.0).astype(BF16)


def joined_rows(product):
    row = lax.broadcasted_iota(jnp.int32, product.shape, 0)
    first = jnp.sum(jnp.where(row < 3, product, 0.0), axis=0, keepdims=True)
    second = jnp.sum(jnp.where((row >= 3) & (row < 6), product, 0.0), axis=0, keepdims=True)
    return first, second


def group_sum(value, per_group):
    lane = lax.broadcasted_iota(jnp.int32, value.shape, 1)
    channels = value.shape[1]
    step = 1
    while step < per_group:
        other = jnp.where(lane & step == 0, pltpu.roll(value, channels - step, 1), pltpu.roll(value, step, 1))
        value = value + other
        step *= 2
    return value


def pack_moments(channel_sum, channel_square, count):
    channels = channel_sum.shape[1]
    per_group = channels // GROUPS
    channel_mean = channel_sum * (1.0 / count)
    group_mean = group_sum(channel_mean, per_group) * (1.0 / per_group)
    spread = channel_mean - group_mean
    square = channel_square + spread * spread * count
    lane = lax.broadcasted_iota(jnp.int32, (channels, LANES), 1)
    group = lax.broadcasted_iota(jnp.int32, (channels, LANES), 0) // per_group
    chosen = ((lane == group) | (lane == group + GROUPS)).astype(F32).astype(BF16)
    product = jnp.dot(split_rows(channel_mean * (1.0 / per_group), square), chosen, preferred_element_type=F32)
    mean, square = joined_rows(product)
    lane = lax.broadcasted_iota(jnp.int32, (1, LANES), 1)
    return jnp.where(lane < GROUPS, mean, square)


def merge_moments(gathered, count, gain, shift, channels):
    devices = gathered.shape[0]
    per_group = channels // GROUPS
    total = jnp.broadcast_to(jnp.sum(gathered, axis=0, keepdims=True), (8, LANES))
    away = gathered - (total * (1.0 / devices))[0:1]
    between = jnp.broadcast_to(jnp.sum(away * away, axis=0, keepdims=True), (8, LANES))
    lane = lax.broadcasted_iota(jnp.int32, (LANES, 2 * channels), 0)
    column = lax.broadcasted_iota(jnp.int32, (LANES, 2 * channels), 1)
    chosen = (lane == column // per_group).astype(F32).astype(BF16)
    product = jnp.dot(split_rows(total, between), chosen, preferred_element_type=F32)
    first, second = joined_rows(product)
    mean = first[:, :channels] * (1.0 / devices)
    within = first[:, channels:]
    variance = (within + second[:, :channels] * count) * (1.0 / (count * devices))
    scale = gain / jnp.sqrt(variance + EPSILON)
    return 0.5 * scale, 0.5 * (shift - mean * scale)


def stats_kernel(values_ref, out_ref, own_ref, arrived, *, devices):
    frames, rows, width, channels = own_ref.shape
    count = frames * rows * width
    copies = [
        [pltpu.make_async_copy(values_ref.at[f, r], own_ref.at[f, r], arrived.at[f, r]) for r in range(rows)]
        for f in range(frames)
    ]
    for f in range(frames):
        for r in range(rows):
            copies[f][r].start()
    acc = jnp.zeros((8, channels), F32)
    for f in range(frames):
        for r in range(rows):
            copies[f][r].wait()
            acc = acc + jnp.sum(own_ref[f, r].astype(F32).reshape(width // 8, 8, channels), axis=0)
    channel_sum = jnp.broadcast_to(jnp.sum(acc, axis=0, keepdims=True), (8, channels))
    mean = channel_sum * (1.0 / count)
    acc = jnp.zeros((8, channels), F32)
    for f in range(frames):
        for r in range(rows):
            away = own_ref[f, r].astype(F32).reshape(width // 8, 8, channels) - mean[None]
            acc = acc + jnp.sum(away * away, axis=0)
    channel_square = jnp.broadcast_to(jnp.sum(acc, axis=0, keepdims=True), (8, channels))
    packed = pack_moments(channel_sum, channel_square, count)
    out_ref[...] = jnp.broadcast_to(packed, (devices, LANES))


def fill_acts(act_ref, own_ref, prior_ref, inter_ref, intra_ref, place_ref, scale, offset, bias):
    width = own_ref.shape[2]
    piece = 64

    def act(block, keep):
        def step(p, _):
            for s in range(2):
                at = pl.ds(pl.multiple_of((p * 2 + s) * (piece // 2), piece // 2), piece // 2)
                yield_at = at
                source, target = block
                v = source[yield_at].astype(F32)
                if bias is not None:
                    v = v + bias[0:1]
                h = v * scale[0:1] + offset[0:1]
                target[yield_at] = ((h + h * jnp.tanh(h)) * keep).astype(BF16)
            return 0

        lax.fori_loop(0, width // piece, step, 0)

    core = place_ref[0]
    frame_keep = place_ref[1].astype(F32)
    inter_keep = place_ref[2].astype(F32)
    inter_row = core * 3
    for f in range(4):
        keep = frame_keep if f < 2 else jnp.float32(1.0)
        source = prior_ref.at[f] if f < 2 else own_ref.at[f - 2]
        for r in range(2):
            act((source.at[r], act_ref.at[f, r + 1]), keep)
        act((inter_ref.at[f], act_ref.at[f, inter_row]), keep * inter_keep)
        act((intra_ref.at[f], act_ref.at[f, 3 - inter_row]), keep)


def conv_frame(act_ref, weight_ref, t):
    width, channels = act_ref.shape[2], act_ref.shape[3]
    q = lax.broadcasted_iota(jnp.int32, (2 * width, channels), 0) % width
    total = None
    for k in (1, 0, 2):
        acc = None
        for i in range(3):
            for j in range(3):
                window = act_ref[t + i, j : j + 2].reshape(2 * width, channels)
                part = jnp.dot(window, weight_ref[i, j, k], preferred_element_type=F32)
                acc = part if acc is None else acc + part
        if k == 0:
            acc = jnp.where(q == 0, 0.0, pltpu.roll(acc, 1, 0))
        elif k == 2:
            acc = jnp.where(q == width - 1, 0.0, pltpu.roll(acc, 2 * width - 1, 0))
        total = acc if total is None else total + acc
    return total


def first_kernel(
    place_ref, own_ref, prior_ref, inter_ref, intra_ref, gathered_ref, vectors_ref, weight_hbm,
    hidden_ref, moments_ref, act_ref, sum_ref, weight_ref, arrived,
):
    t = pl.program_id(0)
    width, channels = own_ref.shape[2], own_ref.shape[3]
    devices = gathered_ref.shape[0]
    per_device = 4 * width * (channels // GROUPS)

    @pl.when(t == 0)
    def _():
        fetch = pltpu.make_async_copy(weight_hbm, weight_ref, arrived)
        fetch.start()
        scale, offset = merge_moments(gathered_ref[...], per_device, vectors_ref[0], vectors_ref[1], channels)
        fill_acts(act_ref, own_ref, prior_ref, inter_ref, intra_ref, place_ref, scale, offset, None)
        fetch.wait()

    hidden = conv_frame(act_ref, weight_ref, t)
    hidden_ref[t] = hidden.reshape(2, width, channels).astype(BF16)
    folded = hidden.reshape(2 * width // 8, 8, channels)
    count = 2.0 * width
    frame_sum = jnp.broadcast_to(jnp.sum(jnp.sum(folded, axis=0), axis=0, keepdims=True), (8, channels))
    frame_mean = frame_sum * (1.0 / count)
    away = folded - frame_mean[None]
    frame_square = jnp.broadcast_to(jnp.sum(jnp.sum(away * away, axis=0), axis=0, keepdims=True), (8, channels))

    @pl.when(t == 0)
    def _():
        sum_ref[0] = frame_sum
        sum_ref[1] = frame_square

    @pl.when(t == 1)
    def _():
        apart = (frame_sum - sum_ref[0]) * (1.0 / count)
        both = frame_sum + sum_ref[0] + (2.0 * count) * vectors_ref[2]
        square = frame_square + sum_ref[1] + apart * apart * (0.5 * count)
        packed = pack_moments(both, square, 2.0 * count)
        moments_ref[...] = jnp.broadcast_to(packed, (devices, LANES))


def second_kernel(
    place_ref, latents_ref, own_ref, prior_ref, inter_ref, intra_ref, gathered_ref, vectors_ref, up_bias_ref, weight_hbm,
    up_hbm, video_ref, act_ref, wide_ref, stage_ref, sent, weight_ref, up_ref, arrived,
):
    t = pl.program_id(0)
    width, channels = own_ref.shape[2], own_ref.shape[3]
    per_device = 4 * width * (channels // GROUPS)

    @pl.when(t == 0)
    def _():
        fetch = pltpu.make_async_copy(weight_hbm, weight_ref, arrived.at[0])
        fetch.start()
        fetch_up = pltpu.make_async_copy(up_hbm, up_ref, arrived.at[1])
        fetch_up.start()
        scale, offset = merge_moments(gathered_ref[...], per_device, vectors_ref[0], vectors_ref[1], channels)
        fill_acts(act_ref, own_ref, prior_ref, inter_ref, intra_ref, place_ref, scale, offset, vectors_ref[2])
        fetch.wait()
        fetch_up.wait()

    def sending(frame, a, b, r):
        return pltpu.make_async_copy(
            stage_ref.at[frame, a, 2 * r + b],
            video_ref.at[2 * frame + a, 2 * r + b],
            sent.at[frame, a, 2 * r + b],
        )

    conv = conv_frame(act_ref, weight_ref, t) + vectors_ref[3]
    latents = latents_ref[t].reshape(2 * width, channels).astype(F32)
    block_out = (latents + conv).astype(BF16)
    for a in range(2):
        for b in range(2):
            for e in range(2):
                n = ((2 * a + b) * 2 + e) * channels
                part = jnp.dot(block_out, up_ref[:, n : n + channels], preferred_element_type=F32)
                part = part + up_bias_ref[:, n : n + channels]
                for lane in range(0, channels, LANES):
                    wide_ref[b, lane // LANES, pl.ds(e, 2 * width, stride=2), :] = part[:, lane : lane + LANES]
            for r in range(2):
                for lane in range(0, channels, LANES):
                    stage_ref[t, a, 2 * r + b, :, lane : lane + LANES] = wide_ref[
                        b, lane // LANES, 2 * width * r : 2 * width * (r + 1), :
                    ].astype(BF16)
                sending(t, a, b, r).start()

    @pl.when(t == 1)
    def _():
        for frame in range(2):
            for a in range(2):
                for b in range(2):
                    for r in range(2):
                        sending(frame, a, b, r).wait()


def edges_kernel(*refs, fetched):
    core_ref, own_ref, prior_ref = refs[:3]
    sources = refs[3 : 3 + fetched]
    outward_ref, inward_ref, vectors_ref = refs[3 + fetched : 6 + fetched]
    targets = refs[6 + fetched : -1]
    arrived = refs[-1]
    vectors = vectors_ref.shape[0]
    copies = [pltpu.make_async_copy(sources[i], vectors_ref.at[i], arrived.at[i]) for i in range(vectors)]
    copies += [
        pltpu.make_async_copy(sources[vectors + i], targets[i], arrived.at[vectors + i]) for i in range(len(targets))
    ]
    for copy in copies:
        copy.start()
    core = core_ref[0]
    for f in range(4):
        source = prior_ref.at[f] if f < 2 else own_ref.at[f - 2]
        outward_ref[f] = source[core]
        inward_ref[f] = source[1 - core]
    for copy in copies:
        copy.wait()


VMEM = pl.BlockSpec(memory_space=pltpu.MemorySpace.VMEM)
HBM = pl.BlockSpec(memory_space=pltpu.MemorySpace.HBM)
SMEM = pl.BlockSpec(memory_space=pltpu.MemorySpace.SMEM)


def in_hbm(x):
    return pltpu.with_memory_space_constraint(x, pltpu.MemorySpace.HBM)


def params(mebibytes):
    return pltpu.CompilerParams(
        dimension_semantics=("arbitrary",), vmem_limit_bytes=mebibytes * 1024 * 1024
    )


def send_on(cells):
    return lax.ppermute(cells, "tm", [(i, i + 1) for i in range(lax.axis_size("tm") - 1)])


def share(moments):
    return lax.all_to_all(moments, EVERY, split_axis=0, concat_axis=0, tiled=True)


def send_edges(cells, prior, place, vectors, weights):
    frames, _, width, channels = cells.shape
    edge = jax.ShapeDtypeStruct((2 * frames, width, channels), BF16)
    vectors = [v.reshape(1, -1) for v in vectors]
    fetched = len(vectors) + len(weights)
    outward, inward, *held = pl.pallas_call(
        functools.partial(edges_kernel, fetched=fetched),
        in_specs=[SMEM, VMEM, VMEM] + [HBM] * fetched,
        out_specs=[VMEM] * (3 + len(weights)),
        out_shape=[edge, edge, jax.ShapeDtypeStruct((len(vectors), 1, channels), F32)]
        + [jax.ShapeDtypeStruct(w.shape, w.dtype) for w in weights],
        scratch_shapes=[pltpu.SemaphoreType.DMA((fetched,))],
        compiler_params=pltpu.CompilerParams(vmem_limit_bytes=1024 * 1024),
    )(place, cells, prior, *map(in_hbm, (*vectors, *weights)))
    rows = lax.axis_size(ROWS)
    between = [(i, i + 1) for i in range(1, rows - 1, 2)] + [(i + 1, i) for i in range(1, rows - 1, 2)]
    within = [(i, i ^ 1) for i in range(rows)]
    inter = lax.ppermute(outward, ROWS, between)
    intra = lax.ppermute(inward, ROWS, within)
    return inter, intra, *held


def body(
    latents,
    norm1_gain,
    norm1_shift,
    conv1_weight,
    conv1_bias,
    norm2_gain,
    norm2_shift,
    conv2_weight,
    conv2_bias,
    up_weight,
    up_bias,
):
    frames, rows, width, channels = latents.shape
    devices = lax.axis_size(EVERY)
    core = lax.axis_index("rows_2")
    row_block = lax.axis_index(ROWS)
    edge = jnp.where(core == 0, row_block == 0, row_block == lax.axis_size(ROWS) - 1)
    place = jnp.stack(
        [core, (lax.axis_index("tm") > 0).astype(jnp.int32), 1 - edge.astype(jnp.int32)]
    ).astype(jnp.int32)
    moments_shape = jax.ShapeDtypeStruct((devices, LANES), F32)
    cells_shape = jax.ShapeDtypeStruct(latents.shape, BF16)
    acts = pltpu.VMEM((2 * frames, rows + 2, width, channels), BF16)

    prior = send_on(latents)
    moments, own = pl.pallas_call(
        functools.partial(stats_kernel, devices=devices),
        in_specs=[HBM],
        out_specs=[VMEM, VMEM],
        out_shape=[moments_shape, cells_shape],
        scratch_shapes=[pltpu.SemaphoreType.DMA((frames, rows))],
        compiler_params=pltpu.CompilerParams(vmem_limit_bytes=1024 * 1024),
    )(in_hbm(latents))
    gathered = share(moments)
    inter, intra, vectors = send_edges(own, prior, place, (norm1_gain, norm1_shift, conv1_bias), ())
    hidden, moments = pl.pallas_call(
        first_kernel,
        grid=(frames,),
        in_specs=[SMEM] + [VMEM] * 6 + [HBM],
        out_specs=[VMEM, VMEM],
        out_shape=[cells_shape, moments_shape],
        scratch_shapes=[
            acts,
            pltpu.VMEM((2, 8, channels), F32),
            pltpu.VMEM(conv1_weight.shape, BF16),
            pltpu.SemaphoreType.DMA(()),
        ],
        compiler_params=params(12),
    )(place, own, prior, inter, intra, gathered, vectors, in_hbm(conv1_weight))

    prior = send_on(hidden)
    gathered = share(moments)
    inter, intra, vectors, up_bias = send_edges(
        hidden, prior, place, (norm2_gain, norm2_shift, conv1_bias, conv2_bias), (up_bias.reshape(1, -1),)
    )
    return pl.pallas_call(
        second_kernel,
        grid=(frames,),
        in_specs=[SMEM] + [VMEM] * 8 + [HBM, HBM],
        out_specs=HBM,
        out_shape=jax.ShapeDtypeStruct((2 * frames, 2 * rows, 2 * width, channels), BF16),
        scratch_shapes=[
            acts,
            pltpu.VMEM((2, channels // LANES, 2 * rows * width, LANES), F32),
            pltpu.VMEM((frames, 2, 2 * rows, 2 * width, channels), BF16),
            pltpu.SemaphoreType.DMA((frames, 2, 2 * rows)),
            pltpu.VMEM(conv2_weight.shape, BF16),
            pltpu.VMEM(up_weight.shape, BF16),
            pltpu.SemaphoreType.DMA((2,)),
        ],
        compiler_params=params(24),
    )(place, own, hidden, prior, inter, intra, gathered, vectors, up_bias, in_hbm(conv2_weight), in_hbm(up_weight))


def solution(mesh):
    finer = Mesh(
        mesh.devices.reshape(mesh.shape["tm"], 8, 4, 2), ("tm", "rows_0", "rows_1", "rows_2")
    )
    placed = (P("tm", ROWS, None, None), P(), P(), P(), P(), P(), P(), P(), P(), P(), P())
    return jax.shard_map(
        body, mesh=finer, in_specs=placed, out_specs=P("tm", ROWS, None, None), check_vma=False
    )
```

```python
import functools

import jax
import jax.numpy as jnp
from jax import lax
from jax.experimental import pallas as pl
from jax.experimental.pallas import tpu as pltpu
from jax.sharding import Mesh
from jax.sharding import PartitionSpec as P


GROUPS = 32
EPSILON = 1e-06
ROWS = ("rows_0", "rows_1", "rows_2")
F32 = jnp.float32
BF16 = jnp.bfloat16
LANES = 128


def split_rows(first, second):
    row = lax.broadcasted_iota(jnp.int32, first.shape, 0)
    value = jnp.where(row < 3, first, second)
    high = value.astype(BF16).astype(F32)
    middle = (value - high).astype(BF16).astype(F32)
    low = value - high - middle
    step = jnp.where(row < 3, row, row - 3)
    part = jnp.where(step == 0, high, jnp.where(step == 1, middle, low))
    return jnp.where(row < 6, part, 0.0).astype(BF16)


def joined_rows(product):
    row = lax.broadcasted_iota(jnp.int32, product.shape, 0)
    first = jnp.sum(jnp.where(row < 3, product, 0.0), axis=0, keepdims=True)
    second = jnp.sum(jnp.where((row >= 3) & (row < 6), product, 0.0), axis=0, keepdims=True)
    return first, second


def group_sum(value, per_group):
    lane = lax.broadcasted_iota(jnp.int32, value.shape, 1)
    channels = value.shape[1]
    step = 1
    while step < per_group:
        other = jnp.where(lane & step == 0, pltpu.roll(value, channels - step, 1), pltpu.roll(value, step, 1))
        value = value + other
        step *= 2
    return value


def pack_moments(channel_sum, channel_square, count):
    channels = channel_sum.shape[1]
    per_group = channels // GROUPS
    channel_mean = channel_sum * (1.0 / count)
    group_mean = group_sum(channel_mean, per_group) * (1.0 / per_group)
    spread = channel_mean - group_mean
    square = channel_square + spread * spread * count
    lane = lax.broadcasted_iota(jnp.int32, (channels, LANES), 1)
    group = lax.broadcasted_iota(jnp.int32, (channels, LANES), 0) // per_group
    chosen = ((lane == group) | (lane == group + GROUPS)).astype(F32).astype(BF16)
    product = jnp.dot(split_rows(channel_mean * (1.0 / per_group), square), chosen, preferred_element_type=F32)
    mean, square = joined_rows(product)
    lane = lax.broadcasted_iota(jnp.int32, (1, LANES), 1)
    return jnp.where(lane < GROUPS, mean, square)


def merge_moments(gathered, count, gain, shift, channels):
    devices = gathered.shape[0]
    per_group = channels // GROUPS
    total = jnp.broadcast_to(jnp.sum(gathered, axis=0, keepdims=True), (8, LANES))
    away = gathered - (total * (1.0 / devices))[0:1]
    between = jnp.broadcast_to(jnp.sum(away * away, axis=0, keepdims=True), (8, LANES))
    lane = lax.broadcasted_iota(jnp.int32, (LANES, 2 * channels), 0)
    column = lax.broadcasted_iota(jnp.int32, (LANES, 2 * channels), 1)
    chosen = (lane == column // per_group).astype(F32).astype(BF16)
    product = jnp.dot(split_rows(total, between), chosen, preferred_element_type=F32)
    first, second = joined_rows(product)
    mean = first[:, :channels] * (1.0 / devices)
    within = first[:, channels:]
    variance = (within + second[:, :channels] * count) * (1.0 / (count * devices))
    scale = gain / jnp.sqrt(variance + EPSILON)
    return 0.5 * scale, 0.5 * (shift - mean * scale)


def merge_kernel(gathered_ref, out_ref, *, count):
    gathered = gathered_ref[...]
    members = gathered.shape[0]
    total = jnp.sum(gathered, axis=0, keepdims=True)
    mean = total * (1.0 / members)
    away = gathered - mean
    between = jnp.broadcast_to(jnp.sum(away * away, axis=0, keepdims=True), (8, LANES))
    square = total + pltpu.roll(between, GROUPS, 1)[0:1] * count
    lane = lax.broadcasted_iota(jnp.int32, (1, LANES), 1)
    out_ref[...] = jnp.broadcast_to(jnp.where(lane < GROUPS, mean, square), out_ref.shape)


def stats_kernel(values_ref, *refs):
    fetched = (len(refs) - 4) // 2
    sources = refs[:fetched]
    out_ref, own_ref = refs[fetched : fetched + 2]
    targets = refs[fetched + 2 : 2 * fetched + 2]
    arrived, vectors_arrived = refs[2 * fetched + 2 :]
    frames, rows, width, channels = own_ref.shape
    count = frames * rows * width
    copies = [
        [pltpu.make_async_copy(values_ref.at[f, r], own_ref.at[f, r], arrived.at[f, r]) for r in range(rows)]
        for f in range(frames)
    ]
    for f in range(frames):
        for r in range(rows):
            copies[f][r].start()
    fetches = [pltpu.make_async_copy(sources[i], targets[i], vectors_arrived.at[i]) for i in range(fetched)]
    for fetch in fetches:
        fetch.start()
    acc = jnp.zeros((8, channels), F32)
    for f in range(frames):
        for r in range(rows):
            copies[f][r].wait()
            acc = acc + jnp.sum(own_ref[f, r].astype(F32).reshape(width // 8, 8, channels), axis=0)
    channel_sum = jnp.broadcast_to(jnp.sum(acc, axis=0, keepdims=True), (8, channels))
    mean = channel_sum * (1.0 / count)
    acc = jnp.zeros((8, channels), F32)
    for f in range(frames):
        for r in range(rows):
            away = own_ref[f, r].astype(F32).reshape(width // 8, 8, channels) - mean[None]
            acc = acc + jnp.sum(away * away, axis=0)
    channel_square = jnp.broadcast_to(jnp.sum(acc, axis=0, keepdims=True), (8, channels))
    packed = pack_moments(channel_sum, channel_square, count)
    out_ref[...] = jnp.broadcast_to(packed, out_ref.shape)
    for fetch in fetches:
        fetch.wait()


def fill_acts(act_ref, own_ref, prior_ref, inter_ref, intra_ref, place_ref, scale, offset, bias):
    width = own_ref.shape[2]
    piece = 64

    def act(block, keep):
        def step(p, _):
            for s in range(2):
                at = pl.ds(pl.multiple_of((p * 2 + s) * (piece // 2), piece // 2), piece // 2)
                yield_at = at
                source, target = block
                v = source[yield_at].astype(F32)
                if bias is not None:
                    v = v + bias[0:1]
                h = v * scale[0:1] + offset[0:1]
                target[yield_at] = ((h + h * jnp.tanh(h)) * keep).astype(BF16)
            return 0

        lax.fori_loop(0, width // piece, step, 0)

    core = place_ref[0]
    frame_keep = place_ref[1].astype(F32)
    inter_keep = place_ref[2].astype(F32)
    inter_row = core * 3
    for f in range(4):
        keep = frame_keep if f < 2 else jnp.float32(1.0)
        source = prior_ref.at[f] if f < 2 else own_ref.at[f - 2]
        for r in range(2):
            act((source.at[r], act_ref.at[f, r + 1]), keep)
        act((inter_ref.at[f], act_ref.at[f, inter_row]), keep * inter_keep)
        act((intra_ref.at[f], act_ref.at[f, 3 - inter_row]), keep)


def conv_frame(act_ref, weight_ref, t):
    width, channels = act_ref.shape[2], act_ref.shape[3]
    q = lax.broadcasted_iota(jnp.int32, (2 * width, channels), 0) % width
    total = None
    for k in (1, 0, 2):
        acc = None
        for i in range(3):
            for j in range(3):
                window = act_ref[t + i, j : j + 2].reshape(2 * width, channels)
                part = jnp.dot(window, weight_ref[i, j, k], preferred_element_type=F32)
                acc = part if acc is None else acc + part
        if k == 0:
            acc = jnp.where(q == 0, 0.0, pltpu.roll(acc, 1, 0))
        elif k == 2:
            acc = jnp.where(q == width - 1, 0.0, pltpu.roll(acc, 2 * width - 1, 0))
        total = acc if total is None else total + acc
    return total


def first_kernel(
    place_ref, own_ref, prior_ref, inter_ref, intra_ref, gathered_ref, gain_ref, shift_ref, bias_ref, weight_hbm,
    hidden_ref, moments_ref, act_ref, sum_ref, weight_ref, arrived, *, count,
):
    t = pl.program_id(0)
    width, channels = own_ref.shape[2], own_ref.shape[3]

    @pl.when(t == 0)
    def _():
        fetch = pltpu.make_async_copy(weight_hbm, weight_ref, arrived)
        fetch.start()
        scale, offset = merge_moments(gathered_ref[...], count, gain_ref[...], shift_ref[...], channels)
        fill_acts(act_ref, own_ref, prior_ref, inter_ref, intra_ref, place_ref, scale, offset, None)
        fetch.wait()

    hidden = conv_frame(act_ref, weight_ref, t)
    hidden_ref[t] = hidden.reshape(2, width, channels).astype(BF16)
    folded = hidden.reshape(2 * width // 8, 8, channels)
    cells = 2.0 * width
    frame_sum = jnp.broadcast_to(jnp.sum(jnp.sum(folded, axis=0), axis=0, keepdims=True), (8, channels))
    frame_mean = frame_sum * (1.0 / cells)
    away = folded - frame_mean[None]
    frame_square = jnp.broadcast_to(jnp.sum(jnp.sum(away * away, axis=0), axis=0, keepdims=True), (8, channels))

    @pl.when(t == 0)
    def _():
        sum_ref[0] = frame_sum
        sum_ref[1] = frame_square

    @pl.when(t == 1)
    def _():
        apart = (frame_sum - sum_ref[0]) * (1.0 / cells)
        both = frame_sum + sum_ref[0] + (2.0 * cells) * bias_ref[...]
        square = frame_square + sum_ref[1] + apart * apart * (0.5 * cells)
        packed = pack_moments(both, square, 2.0 * cells)
        moments_ref[...] = jnp.broadcast_to(packed, moments_ref.shape)


def second_kernel(
    place_ref, latents_ref, own_ref, prior_ref, inter_ref, intra_ref, gathered_ref, gain_ref, shift_ref, bias1_ref,
    bias2_ref, up_bias_ref, weight_hbm, up_hbm, video_ref, act_ref, wide_ref, stage_ref, sent, weight_ref, up_ref,
    arrived, *, count,
):
    t = pl.program_id(0)
    width, channels = own_ref.shape[2], own_ref.shape[3]

    @pl.when(t == 0)
    def _():
        fetch = pltpu.make_async_copy(weight_hbm, weight_ref, arrived.at[0])
        fetch.start()
        fetch_up = pltpu.make_async_copy(up_hbm, up_ref, arrived.at[1])
        fetch_up.start()
        scale, offset = merge_moments(gathered_ref[...], count, gain_ref[...], shift_ref[...], channels)
        fill_acts(act_ref, own_ref, prior_ref, inter_ref, intra_ref, place_ref, scale, offset, bias1_ref[...])
        fetch.wait()
        fetch_up.wait()

    def sending(frame, a, b, r):
        return pltpu.make_async_copy(
            stage_ref.at[frame, a, 2 * r + b],
            video_ref.at[2 * frame + a, 2 * r + b],
            sent.at[frame, a, 2 * r + b],
        )

    conv = conv_frame(act_ref, weight_ref, t) + bias2_ref[...]
    latents = latents_ref[t].reshape(2 * width, channels).astype(F32)
    block_out = (latents + conv).astype(BF16)
    for a in range(2):
        for b in range(2):
            for e in range(2):
                n = ((2 * a + b) * 2 + e) * channels
                part = jnp.dot(block_out, up_ref[:, n : n + channels], preferred_element_type=F32)
                part = part + up_bias_ref[:, n : n + channels]
                for lane in range(0, channels, LANES):
                    wide_ref[b, lane // LANES, pl.ds(e, 2 * width, stride=2), :] = part[:, lane : lane + LANES]
            for r in range(2):
                for lane in range(0, channels, LANES):
                    stage_ref[t, a, 2 * r + b, :, lane : lane + LANES] = wide_ref[
                        b, lane // LANES, 2 * width * r : 2 * width * (r + 1), :
                    ].astype(BF16)
                sending(t, a, b, r).start()

    @pl.when(t == 1)
    def _():
        for frame in range(2):
            for a in range(2):
                for b in range(2):
                    for r in range(2):
                        sending(frame, a, b, r).wait()


def edges_kernel(place_ref, own_ref, prior_ref, outward_ref, inward_ref):
    core = place_ref[0]
    for f in range(4):
        source = prior_ref.at[f] if f < 2 else own_ref.at[f - 2]
        outward_ref[f] = source[core]
        inward_ref[f] = source[1 - core]


VMEM = pl.BlockSpec(memory_space=pltpu.MemorySpace.VMEM)
HBM = pl.BlockSpec(memory_space=pltpu.MemorySpace.HBM)
SMEM = pl.BlockSpec(memory_space=pltpu.MemorySpace.SMEM)


def in_hbm(x):
    return pltpu.with_memory_space_constraint(x, pltpu.MemorySpace.HBM)


def params(mebibytes):
    return pltpu.CompilerParams(
        dimension_semantics=("arbitrary",), vmem_limit_bytes=mebibytes * 1024 * 1024
    )


def send_on(cells):
    return lax.ppermute(cells, "tm", [(i, i + 1) for i in range(lax.axis_size("tm") - 1)])


FIRST = ROWS
SECOND = "tm"


def share(moments, axes):
    return lax.all_to_all(moments, axes, split_axis=0, concat_axis=0, tiled=True)


def share_all(moments, count):
    first = share(moments, FIRST)
    merged = pl.pallas_call(
        functools.partial(merge_kernel, count=count),
        in_specs=[VMEM],
        out_specs=VMEM,
        out_shape=jax.ShapeDtypeStruct((lax.axis_size(SECOND), LANES), F32),
        compiler_params=pltpu.CompilerParams(vmem_limit_bytes=1024 * 1024),
    )(first)
    return share(merged, SECOND)


def send_edges(cells, prior, place):
    frames, _, width, channels = cells.shape
    edge = jax.ShapeDtypeStruct((2 * frames, width, channels), BF16)
    outward, inward = pl.pallas_call(
        edges_kernel,
        in_specs=[SMEM, VMEM, VMEM],
        out_specs=[VMEM, VMEM],
        out_shape=[edge, edge],
        compiler_params=pltpu.CompilerParams(vmem_limit_bytes=1024 * 1024),
    )(place, cells, prior)
    rows = lax.axis_size(ROWS)
    between = [(i, i + 1) for i in range(1, rows - 1, 2)] + [(i + 1, i) for i in range(1, rows - 1, 2)]
    within = [(i, i ^ 1) for i in range(rows)]
    inter = lax.ppermute(outward, ROWS, between)
    intra = lax.ppermute(inward, ROWS, within)
    return inter, intra


def body(
    latents,
    norm1_gain,
    norm1_shift,
    conv1_weight,
    conv1_bias,
    norm2_gain,
    norm2_shift,
    conv2_weight,
    conv2_bias,
    up_weight,
    up_bias,
):
    frames, rows, width, channels = latents.shape
    core = lax.axis_index("rows_2")
    row_block = lax.axis_index(ROWS)
    edge = jnp.where(core == 0, row_block == 0, row_block == lax.axis_size(ROWS) - 1)
    place = jnp.stack(
        [core, (lax.axis_index("tm") > 0).astype(jnp.int32), 1 - edge.astype(jnp.int32)]
    ).astype(jnp.int32)
    moments_shape = jax.ShapeDtypeStruct((lax.axis_size(FIRST), LANES), F32)
    cells_shape = jax.ShapeDtypeStruct(latents.shape, BF16)
    acts = pltpu.VMEM((2 * frames, rows + 2, width, channels), BF16)
    one_device = frames * rows * width * (channels // GROUPS)
    one_row = one_device * lax.axis_size(FIRST)
    vectors = (norm1_gain, norm1_shift, conv1_bias, norm2_gain, norm2_shift, conv2_bias, up_bias)
    vectors = [v.reshape(1, -1) for v in vectors]

    prior = send_on(latents)
    moments, own, gain1, shift1, bias1, gain2, shift2, bias2, bias_up = pl.pallas_call(
        stats_kernel,
        in_specs=[HBM] * (1 + len(vectors)),
        out_specs=[VMEM] * (2 + len(vectors)),
        out_shape=[moments_shape, cells_shape] + [jax.ShapeDtypeStruct(v.shape, F32) for v in vectors],
        scratch_shapes=[
            pltpu.SemaphoreType.DMA((frames, rows)),
            pltpu.SemaphoreType.DMA((len(vectors),)),
        ],
        compiler_params=pltpu.CompilerParams(vmem_limit_bytes=1024 * 1024),
    )(*map(in_hbm, (latents, *vectors)))
    inter, intra = send_edges(own, prior, place)
    gathered = share_all(moments, one_device)
    hidden, moments = pl.pallas_call(
        functools.partial(first_kernel, count=one_row),
        grid=(frames,),
        in_specs=[SMEM] + [VMEM] * 8 + [HBM],
        out_specs=[VMEM, VMEM],
        out_shape=[cells_shape, moments_shape],
        scratch_shapes=[
            acts,
            pltpu.VMEM((2, 8, channels), F32),
            pltpu.VMEM(conv1_weight.shape, BF16),
            pltpu.SemaphoreType.DMA(()),
        ],
        compiler_params=params(12),
    )(place, own, prior, inter, intra, gathered, gain1, shift1, bias1, in_hbm(conv1_weight))

    prior = send_on(hidden)
    inter, intra = send_edges(hidden, prior, place)
    gathered = share_all(moments, one_device)
    return pl.pallas_call(
        functools.partial(second_kernel, count=one_row),
        grid=(frames,),
        in_specs=[SMEM] + [VMEM] * 11 + [HBM, HBM],
        out_specs=HBM,
        out_shape=jax.ShapeDtypeStruct((2 * frames, 2 * rows, 2 * width, channels), BF16),
        scratch_shapes=[
            acts,
            pltpu.VMEM((2, channels // LANES, 2 * rows * width, LANES), F32),
            pltpu.VMEM((frames, 2, 2 * rows, 2 * width, channels), BF16),
            pltpu.SemaphoreType.DMA((frames, 2, 2 * rows)),
            pltpu.VMEM(conv2_weight.shape, BF16),
            pltpu.VMEM(up_weight.shape, BF16),
            pltpu.SemaphoreType.DMA((2,)),
        ],
        compiler_params=params(24),
    )(
        place, own, hidden, prior, inter, intra, gathered, gain2, shift2, bias1, bias2, bias_up,
        in_hbm(conv2_weight), in_hbm(up_weight),
    )


def solution(mesh):
    finer = Mesh(
        mesh.devices.reshape(mesh.shape["tm"], 8, 4, 2), ("tm", "rows_0", "rows_1", "rows_2")
    )
    placed = (P("tm", ROWS, None, None), P(), P(), P(), P(), P(), P(), P(), P(), P(), P())
    return jax.shard_map(
        body, mesh=finer, in_specs=placed, out_specs=P("tm", ROWS, None, None), check_vma=False
    )
```

```python
import functools

import jax
import jax.numpy as jnp
from jax import lax
from jax.experimental import pallas as pl
from jax.experimental.pallas import tpu as pltpu
from jax.sharding import Mesh
from jax.sharding import PartitionSpec as P


GROUPS = 32
EPSILON = 1e-06
ROWS = ("rows_0", "rows_1", "rows_2")
F32 = jnp.float32
BF16 = jnp.bfloat16
LANES = 128


def split_rows(first, second):
    row = lax.broadcasted_iota(jnp.int32, first.shape, 0)
    value = jnp.where(row < 3, first, second)
    high = value.astype(BF16).astype(F32)
    middle = (value - high).astype(BF16).astype(F32)
    low = value - high - middle
    step = jnp.where(row < 3, row, row - 3)
    part = jnp.where(step == 0, high, jnp.where(step == 1, middle, low))
    return jnp.where(row < 6, part, 0.0).astype(BF16)


def joined_rows(product):
    row = lax.broadcasted_iota(jnp.int32, product.shape, 0)
    first = jnp.sum(jnp.where(row < 3, product, 0.0), axis=0, keepdims=True)
    second = jnp.sum(jnp.where((row >= 3) & (row < 6), product, 0.0), axis=0, keepdims=True)
    return first, second


def group_sum(value, per_group):
    lane = lax.broadcasted_iota(jnp.int32, value.shape, 1)
    channels = value.shape[1]
    step = 1
    while step < per_group:
        other = jnp.where(lane & step == 0, pltpu.roll(value, channels - step, 1), pltpu.roll(value, step, 1))
        value = value + other
        step *= 2
    return value


def pack_moments(channel_sum, channel_square, count):
    channels = channel_sum.shape[1]
    per_group = channels // GROUPS
    channel_mean = channel_sum * (1.0 / count)
    group_mean = group_sum(channel_mean, per_group) * (1.0 / per_group)
    spread = channel_mean - group_mean
    square = channel_square + spread * spread * count
    lane = lax.broadcasted_iota(jnp.int32, (channels, LANES), 1)
    group = lax.broadcasted_iota(jnp.int32, (channels, LANES), 0) // per_group
    chosen = ((lane == group) | (lane == group + GROUPS)).astype(F32).astype(BF16)
    product = jnp.dot(split_rows(channel_mean * (1.0 / per_group), square), chosen, preferred_element_type=F32)
    mean, square = joined_rows(product)
    lane = lax.broadcasted_iota(jnp.int32, (1, LANES), 1)
    return jnp.where(lane < GROUPS, mean, square)


def merge_moments(gathered, count, gain, shift, channels):
    devices = gathered.shape[0]
    per_group = channels // GROUPS
    total = jnp.broadcast_to(jnp.sum(gathered, axis=0, keepdims=True), (8, LANES))
    away = gathered - (total * (1.0 / devices))[0:1]
    between = jnp.broadcast_to(jnp.sum(away * away, axis=0, keepdims=True), (8, LANES))
    lane = lax.broadcasted_iota(jnp.int32, (LANES, 2 * channels), 0)
    column = lax.broadcasted_iota(jnp.int32, (LANES, 2 * channels), 1)
    chosen = (lane == column // per_group).astype(F32).astype(BF16)
    product = jnp.dot(split_rows(total, between), chosen, preferred_element_type=F32)
    first, second = joined_rows(product)
    mean = first[:, :channels] * (1.0 / devices)
    within = first[:, channels:]
    variance = (within + second[:, :channels] * count) * (1.0 / (count * devices))
    scale = gain / jnp.sqrt(variance + EPSILON)
    return 0.5 * scale, 0.5 * (shift - mean * scale)


def merge_kernel(gathered_ref, out_ref, *, count):
    gathered = gathered_ref[...]
    members = gathered.shape[0]
    total = jnp.sum(gathered, axis=0, keepdims=True)
    mean = total * (1.0 / members)
    away = gathered - mean
    between = jnp.broadcast_to(jnp.sum(away * away, axis=0, keepdims=True), (8, LANES))
    square = total + pltpu.roll(between, GROUPS, 1)[0:1] * count
    lane = lax.broadcasted_iota(jnp.int32, (1, LANES), 1)
    out_ref[...] = jnp.broadcast_to(jnp.where(lane < GROUPS, mean, square), out_ref.shape)


def stats_kernel(values_ref, *refs):
    fetched = (len(refs) - 4) // 2
    sources = refs[:fetched]
    out_ref, own_ref = refs[fetched : fetched + 2]
    targets = refs[fetched + 2 : 2 * fetched + 2]
    arrived, vectors_arrived = refs[2 * fetched + 2 :]
    frames, rows, width, channels = own_ref.shape
    count = frames * rows * width
    copies = [
        [pltpu.make_async_copy(values_ref.at[f, r], own_ref.at[f, r], arrived.at[f, r]) for r in range(rows)]
        for f in range(frames)
    ]
    for f in range(frames):
        for r in range(rows):
            copies[f][r].start()
    fetches = [pltpu.make_async_copy(sources[i], targets[i], vectors_arrived.at[i]) for i in range(fetched)]
    for fetch in fetches:
        fetch.start()
    acc = jnp.zeros((8, channels), F32)
    for f in range(frames):
        for r in range(rows):
            copies[f][r].wait()
            acc = acc + jnp.sum(own_ref[f, r].astype(F32).reshape(width // 8, 8, channels), axis=0)
    channel_sum = jnp.broadcast_to(jnp.sum(acc, axis=0, keepdims=True), (8, channels))
    mean = channel_sum * (1.0 / count)
    acc = jnp.zeros((8, channels), F32)
    for f in range(frames):
        for r in range(rows):
            away = own_ref[f, r].astype(F32).reshape(width // 8, 8, channels) - mean[None]
            acc = acc + jnp.sum(away * away, axis=0)
    channel_square = jnp.broadcast_to(jnp.sum(acc, axis=0, keepdims=True), (8, channels))
    packed = pack_moments(channel_sum, channel_square, count)
    out_ref[...] = jnp.broadcast_to(packed, out_ref.shape)
    for fetch in fetches:
        fetch.wait()


PIECE = 64
PAD = 8


def position():
    core = lax.axis_index("rows_2")
    row_block = lax.axis_index(ROWS)
    last = lax.axis_size(ROWS) - 1
    inter_exists = jnp.where(core == 0, row_block > 0, row_block < last)
    frames_exist = lax.axis_index("tm") > 0
    return core, jnp.where(frames_exist, 1.0, 0.0).astype(F32), jnp.where(inter_exists, 1.0, 0.0).astype(F32)


def act_steps(f, act_ref, sources, place, scale, offset, bias):
    own_ref, prior_ref, inter_ref, intra_ref = sources
    core, frames_exist, inter_exists = place
    width = own_ref.shape[2]
    half = PIECE // 2
    source = prior_ref.at[f] if f < 2 else own_ref.at[f - 2]
    keep = frames_exist if f < 2 else None
    inter_keep = inter_exists if keep is None else keep * inter_exists
    blocks = [
        (inter_ref.at[f], core * 3, inter_keep),
        (source.at[0], 1, keep),
        (source.at[1], 2, keep),
        (intra_ref.at[f], 3 - core * 3, keep),
    ]

    def step(block, at):
        cells, row, keep = block
        v = cells[at : at + half].astype(F32)
        if bias is not None:
            v = v + bias
        h = v * scale + offset
        silu = h + h * jnp.tanh(h)
        if keep is not None:
            silu = silu * keep
        act_ref[row, at : at + half] = silu.astype(BF16)

    return [functools.partial(step, block, at) for block in blocks for at in range(0, width, half)]


def conv_steps(act_ref, weight_ref, i, sums_ref):
    width, channels = act_ref.shape[1], act_ref.shape[2]

    def step(k):
        part = None
        for j in range(3):
            window = act_ref[j : j + 2].reshape(2 * width, channels)
            product = jnp.dot(window, weight_ref[i, j, k], preferred_element_type=F32)
            part = product if part is None else part + product
        for r in range(2):
            row = part[r * width : (r + 1) * width]
            if i > 0:
                row = row + sums_ref[k, r, PAD : PAD + width]
            sums_ref[k, r, PAD : PAD + width] = row

    return [functools.partial(step, k) for k in range(3)]


def clear_pads(sums_ref):
    width = sums_ref.shape[2] - 2 * PAD
    channels = sums_ref.shape[3]
    for r in range(2):
        sums_ref[0, r, 0:PAD] = jnp.zeros((PAD, channels), F32)
        sums_ref[2, r, PAD + width :] = jnp.zeros((PAD, channels), F32)


def piece_of(sums_ref, r, at):
    left = sums_ref[0, r, PAD + at - 1 : PAD + at - 1 + PIECE]
    middle = sums_ref[1, r, PAD + at : PAD + at + PIECE]
    right = sums_ref[2, r, PAD + at + 1 : PAD + at + 1 + PIECE]
    return middle + left + right


def beside(main, other):
    done = 0
    for n, step in enumerate(main):
        step()
        until = len(other) * (n + 1) // len(main)
        for extra in other[done:until]:
            extra()
        done = until


def run(steps):
    for step in steps:
        step()


def first_kernel(
    own_ref, prior_ref, inter_ref, intra_ref, gathered_ref, gain_ref, shift_ref, bias_ref, weight_hbm,
    hidden_ref, moments_ref, *scratch, count,
):
    acts, sums, (weight_ref, arrived) = scratch[:4], scratch[4:6], scratch[6:]
    width, channels = own_ref.shape[2], own_ref.shape[3]
    fetch = pltpu.make_async_copy(weight_hbm, weight_ref, arrived)
    fetch.start()
    for ref in sums:
        clear_pads(ref)
    scale, offset = merge_moments(gathered_ref[...], count, gain_ref[...], shift_ref[...], channels)
    place = position()
    sources = (own_ref, prior_ref, inter_ref, intra_ref)
    acting = [act_steps(f, acts[f], sources, place, scale, offset, None) for f in range(4)]
    totals = {}

    def finish(t, r, at):
        piece = piece_of(sums[t], r, at)
        hidden_ref[t, r, at : at + PIECE] = piece.astype(BF16)
        if not totals:
            totals["pivot"] = jnp.sum(piece, axis=0, keepdims=True) * (1.0 / PIECE)
            totals["sum"] = jnp.zeros((8, channels), F32)
            totals["square"] = jnp.zeros((8, channels), F32)
        away = (piece - totals["pivot"]).reshape(PIECE // 8, 8, channels)
        totals["sum"] = totals["sum"] + jnp.sum(away, axis=0)
        totals["square"] = totals["square"] + jnp.sum(away * away, axis=0)

    def finishing(t):
        return [functools.partial(finish, t, r, at) for r in range(2) for at in range(0, width, PIECE)]

    taps = lambda f, t: conv_steps(acts[f], weight_ref, f - t, sums[t])
    run(acting[0])
    fetch.wait()
    beside(taps(0, 0), acting[1])
    beside(taps(1, 0) + taps(1, 1), acting[2])
    beside(taps(2, 0) + taps(2, 1), acting[3])
    beside(taps(3, 1), finishing(0))
    run(finishing(1))

    cells = 4.0 * width
    away = jnp.broadcast_to(jnp.sum(totals["sum"], axis=0, keepdims=True), (8, channels))
    square = jnp.broadcast_to(jnp.sum(totals["square"], axis=0, keepdims=True), (8, channels))
    square = jnp.maximum(square - away * away * (1.0 / cells), 0.0)
    total = away + cells * (totals["pivot"] + bias_ref[...])
    moments_ref[...] = jnp.broadcast_to(pack_moments(total, square, cells), moments_ref.shape)


def second_kernel(
    latents_ref, own_ref, prior_ref, inter_ref, intra_ref, gathered_ref, gain_ref, shift_ref, bias1_ref, bias2_ref,
    up_bias_ref, weight_hbm, up_hbm, video_ref, *scratch, count,
):
    acts, sums = scratch[:4], scratch[4:6]
    wide_ref, block_ref, stage_ref, sent, weight_ref, up_ref, arrived = scratch[6:]
    width, channels = own_ref.shape[2], own_ref.shape[3]
    fetch = pltpu.make_async_copy(weight_hbm, weight_ref, arrived.at[0])
    fetch.start()
    fetch_up = pltpu.make_async_copy(up_hbm, up_ref, arrived.at[1])
    fetch_up.start()
    for ref in sums:
        clear_pads(ref)
    scale, offset = merge_moments(gathered_ref[...], count, gain_ref[...], shift_ref[...], channels)
    place = position()
    sources = (own_ref, prior_ref, inter_ref, intra_ref)
    acting = [act_steps(f, acts[f], sources, place, scale, offset, bias1_ref[...]) for f in range(4)]

    def sending(t, a, b, r):
        return pltpu.make_async_copy(
            stage_ref.at[t, a, 2 * r + b], video_ref.at[2 * t + a, 2 * r + b], sent.at[t, a, 2 * r + b]
        )

    def finish(t, r, at):
        latents = latents_ref[t, r, at : at + PIECE].astype(F32)
        block = latents + (piece_of(sums[t], r, at) + bias2_ref[...])
        block_ref[t, r * width + at : r * width + at + PIECE] = block.astype(BF16)

    def finishing(t):
        return [functools.partial(finish, t, r, at) for r in range(2) for at in range(0, width, PIECE)]

    def widen(t, a, b, e):
        n = ((2 * a + b) * 2 + e) * channels
        part = jnp.dot(block_ref[t], up_ref[:, n : n + channels], preferred_element_type=F32)
        part = part + up_bias_ref[:, n : n + channels]
        for lane in range(0, channels, LANES):
            wide_ref[2 * a + b, lane // LANES, pl.ds(e, 2 * width, stride=2), :] = part[:, lane : lane + LANES]

    def send(t, a, b):
        for r in range(2):
            for lane in range(0, channels, LANES):
                stage_ref[t, a, 2 * r + b, :, lane : lane + LANES] = wide_ref[
                    2 * a + b, lane // LANES, 2 * width * r : 2 * width * (r + 1), :
                ].astype(BF16)
            sending(t, a, b, r).start()

    def widening(t):
        steps = []
        for a in range(2):
            for b in range(2):
                steps += [functools.partial(widen, t, a, b, e) for e in range(2)]
                steps.append(functools.partial(send, t, a, b))
        return steps

    taps = lambda f, t: conv_steps(acts[f], weight_ref, f - t, sums[t])
    run(acting[0])
    fetch.wait()
    beside(taps(0, 0), acting[1])
    beside(taps(1, 0) + taps(1, 1), acting[2])
    run(taps(2, 0))
    beside(taps(2, 1), acting[3] + finishing(0))
    fetch_up.wait()
    beside(taps(3, 1), widening(0))
    run(finishing(1))
    run(widening(1))
    for t in range(2):
        for a in range(2):
            for b in range(2):
                for r in range(2):
                    sending(t, a, b, r).wait()


def edges_kernel(own_ref, prior_ref, outward_ref, inward_ref):
    core = lax.axis_index("rows_2")
    for f in range(4):
        source = prior_ref.at[f] if f < 2 else own_ref.at[f - 2]
        outward_ref[f] = source[core]
        inward_ref[f] = source[1 - core]


VMEM = pl.BlockSpec(memory_space=pltpu.MemorySpace.VMEM)
HBM = pl.BlockSpec(memory_space=pltpu.MemorySpace.HBM)


def in_hbm(x):
    return pltpu.with_memory_space_constraint(x, pltpu.MemorySpace.HBM)


def params(mebibytes):
    return pltpu.CompilerParams(
        vmem_limit_bytes=mebibytes * 1024 * 1024
    )


def send_on(cells):
    return lax.ppermute(cells, "tm", [(i, i + 1) for i in range(lax.axis_size("tm") - 1)])


FIRST = ROWS
SECOND = "tm"


def share(moments, axes):
    return lax.all_to_all(moments, axes, split_axis=0, concat_axis=0, tiled=True)


def share_all(moments, count):
    first = share(moments, FIRST)
    merged = pl.pallas_call(
        functools.partial(merge_kernel, count=count),
        in_specs=[VMEM],
        out_specs=VMEM,
        out_shape=jax.ShapeDtypeStruct((lax.axis_size(SECOND), LANES), F32),
        compiler_params=pltpu.CompilerParams(vmem_limit_bytes=1024 * 1024),
    )(first)
    return share(merged, SECOND)


def send_edges(cells, prior):
    frames, _, width, channels = cells.shape
    edge = jax.ShapeDtypeStruct((2 * frames, width, channels), BF16)
    outward, inward = pl.pallas_call(
        edges_kernel,
        in_specs=[VMEM, VMEM],
        out_specs=[VMEM, VMEM],
        out_shape=[edge, edge],
        compiler_params=pltpu.CompilerParams(vmem_limit_bytes=1024 * 1024),
    )(cells, prior)
    rows = lax.axis_size(ROWS)
    between = [(i, i + 1) for i in range(1, rows - 1, 2)] + [(i + 1, i) for i in range(1, rows - 1, 2)]
    within = [(i, i ^ 1) for i in range(rows)]
    inter = lax.ppermute(outward, ROWS, between)
    intra = lax.ppermute(inward, ROWS, within)
    return inter, intra


def body(
    latents,
    norm1_gain,
    norm1_shift,
    conv1_weight,
    conv1_bias,
    norm2_gain,
    norm2_shift,
    conv2_weight,
    conv2_bias,
    up_weight,
    up_bias,
):
    frames, rows, width, channels = latents.shape
    moments_shape = jax.ShapeDtypeStruct((lax.axis_size(FIRST), LANES), F32)
    cells_shape = jax.ShapeDtypeStruct(latents.shape, BF16)
    acts = [pltpu.VMEM((rows + 2, width, channels), BF16)] * (2 * frames)
    sums = [pltpu.VMEM((3, rows, width + 2 * PAD, channels), F32)] * frames
    one_device = frames * rows * width * (channels // GROUPS)
    one_row = one_device * lax.axis_size(FIRST)
    vectors = (norm1_gain, norm1_shift, conv1_bias, norm2_gain, norm2_shift, conv2_bias, up_bias)
    vectors = [v.reshape(1, -1) for v in vectors]

    prior = send_on(latents)
    moments, own, gain1, shift1, bias1, gain2, shift2, bias2, bias_up = pl.pallas_call(
        stats_kernel,
        in_specs=[HBM] * (1 + len(vectors)),
        out_specs=[VMEM] * (2 + len(vectors)),
        out_shape=[moments_shape, cells_shape] + [jax.ShapeDtypeStruct(v.shape, F32) for v in vectors],
        scratch_shapes=[
            pltpu.SemaphoreType.DMA((frames, rows)),
            pltpu.SemaphoreType.DMA((len(vectors),)),
        ],
        compiler_params=pltpu.CompilerParams(vmem_limit_bytes=1024 * 1024),
    )(*map(in_hbm, (latents, *vectors)))
    inter, intra = send_edges(own, prior)
    gathered = share_all(moments, one_device)
    hidden, moments = pl.pallas_call(
        functools.partial(first_kernel, count=one_row),
        in_specs=[VMEM] * 8 + [HBM],
        out_specs=[VMEM, VMEM],
        out_shape=[cells_shape, moments_shape],
        scratch_shapes=[
            *acts,
            *sums,
            pltpu.VMEM(conv1_weight.shape, BF16),
            pltpu.SemaphoreType.DMA(()),
        ],
        compiler_params=params(20),
    )(own, prior, inter, intra, gathered, gain1, shift1, bias1, in_hbm(conv1_weight))

    prior = send_on(hidden)
    inter, intra = send_edges(hidden, prior)
    gathered = share_all(moments, one_device)
    return pl.pallas_call(
        functools.partial(second_kernel, count=one_row),
        in_specs=[VMEM] * 11 + [HBM, HBM],
        out_specs=HBM,
        out_shape=jax.ShapeDtypeStruct((2 * frames, 2 * rows, 2 * width, channels), BF16),
        scratch_shapes=[
            *acts,
            *sums,
            pltpu.VMEM((4, channels // LANES, 2 * rows * width, LANES), F32),
            pltpu.VMEM((frames, rows * width, channels), BF16),
            pltpu.VMEM((frames, 2, 2 * rows, 2 * width, channels), BF16),
            pltpu.SemaphoreType.DMA((frames, 2, 2 * rows)),
            pltpu.VMEM(conv2_weight.shape, BF16),
            pltpu.VMEM(up_weight.shape, BF16),
            pltpu.SemaphoreType.DMA((2,)),
        ],
        compiler_params=params(32),
    )(
        own, hidden, prior, inter, intra, gathered, gain2, shift2, bias1, bias2, bias_up,
        in_hbm(conv2_weight), in_hbm(up_weight),
    )


def solution(mesh):
    finer = Mesh(
        mesh.devices.reshape(mesh.shape["tm"], 8, 4, 2), ("tm", "rows_0", "rows_1", "rows_2")
    )
    placed = (P("tm", ROWS, None, None), P(), P(), P(), P(), P(), P(), P(), P(), P(), P())
    return jax.shard_map(
        body, mesh=finer, in_specs=placed, out_specs=P("tm", ROWS, None, None), check_vma=False
    )
```

```python
import functools

import jax
import jax.numpy as jnp
from jax import lax
from jax.experimental import pallas as pl
from jax.experimental.pallas import tpu as pltpu
from jax.sharding import Mesh
from jax.sharding import PartitionSpec as P


GROUPS = 32
EPSILON = 1e-06
ROWS = ("rows_0", "rows_1", "rows_2")
F32 = jnp.float32
BF16 = jnp.bfloat16
LANES = 128


def split_rows(first, second):
    row = lax.broadcasted_iota(jnp.int32, first.shape, 0)
    value = jnp.where(row < 3, first, second)
    high = value.astype(BF16).astype(F32)
    middle = (value - high).astype(BF16).astype(F32)
    low = value - high - middle
    step = jnp.where(row < 3, row, row - 3)
    part = jnp.where(step == 0, high, jnp.where(step == 1, middle, low))
    return jnp.where(row < 6, part, 0.0).astype(BF16)


def joined_rows(product):
    row = lax.broadcasted_iota(jnp.int32, product.shape, 0)
    first = jnp.sum(jnp.where(row < 3, product, 0.0), axis=0, keepdims=True)
    second = jnp.sum(jnp.where((row >= 3) & (row < 6), product, 0.0), axis=0, keepdims=True)
    return first, second


def group_sum(value, per_group):
    lane = lax.broadcasted_iota(jnp.int32, value.shape, 1)
    channels = value.shape[1]
    step = 1
    while step < per_group:
        other = jnp.where(lane & step == 0, pltpu.roll(value, channels - step, 1), pltpu.roll(value, step, 1))
        value = value + other
        step *= 2
    return value


def pack_moments(channel_sum, channel_square, count):
    channels = channel_sum.shape[1]
    per_group = channels // GROUPS
    channel_mean = channel_sum * (1.0 / count)
    group_mean = group_sum(channel_mean, per_group) * (1.0 / per_group)
    spread = channel_mean - group_mean
    square = channel_square + spread * spread * count
    lane = lax.broadcasted_iota(jnp.int32, (channels, LANES), 1)
    group = lax.broadcasted_iota(jnp.int32, (channels, LANES), 0) // per_group
    chosen = ((lane == group) | (lane == group + GROUPS)).astype(F32).astype(BF16)
    product = jnp.dot(split_rows(channel_mean * (1.0 / per_group), square), chosen, preferred_element_type=F32)
    mean, square = joined_rows(product)
    lane = lax.broadcasted_iota(jnp.int32, (1, LANES), 1)
    return jnp.where(lane < GROUPS, mean, square)


def merge_moments(gathered, count, gain, shift, channels):
    devices = gathered.shape[0]
    per_group = channels // GROUPS
    total = jnp.broadcast_to(jnp.sum(gathered, axis=0, keepdims=True), (8, LANES))
    away = gathered - (total * (1.0 / devices))[0:1]
    between = jnp.broadcast_to(jnp.sum(away * away, axis=0, keepdims=True), (8, LANES))
    lane = lax.broadcasted_iota(jnp.int32, (LANES, 2 * channels), 0)
    column = lax.broadcasted_iota(jnp.int32, (LANES, 2 * channels), 1)
    chosen = (lane == column // per_group).astype(F32).astype(BF16)
    product = jnp.dot(split_rows(total, between), chosen, preferred_element_type=F32)
    first, second = joined_rows(product)
    mean = first[:, :channels] * (1.0 / devices)
    within = first[:, channels:]
    variance = (within + second[:, :channels] * count) * (1.0 / (count * devices))
    scale = gain / jnp.sqrt(variance + EPSILON)
    return 0.5 * scale, 0.5 * (shift - mean * scale)


def merge_kernel(gathered_ref, out_ref, *, count):
    gathered = gathered_ref[...]
    members = gathered.shape[0]
    total = jnp.sum(gathered, axis=0, keepdims=True)
    mean = total * (1.0 / members)
    away = gathered - mean
    between = jnp.broadcast_to(jnp.sum(away * away, axis=0, keepdims=True), (8, LANES))
    square = total + pltpu.roll(between, GROUPS, 1)[0:1] * count
    lane = lax.broadcasted_iota(jnp.int32, (1, LANES), 1)
    out_ref[...] = jnp.broadcast_to(jnp.where(lane < GROUPS, mean, square), out_ref.shape)


def stats_kernel(values_ref, *refs):
    fetched = (len(refs) - 4) // 2
    sources = refs[:fetched]
    out_ref, own_ref = refs[fetched : fetched + 2]
    targets = refs[fetched + 2 : 2 * fetched + 2]
    arrived, vectors_arrived = refs[2 * fetched + 2 :]
    frames, rows, width, channels = own_ref.shape
    count = frames * rows * width
    copies = [
        [pltpu.make_async_copy(values_ref.at[f, r], own_ref.at[f, r], arrived.at[f, r]) for r in range(rows)]
        for f in range(frames)
    ]
    for f in range(frames):
        for r in range(rows):
            copies[f][r].start()
    fetches = [pltpu.make_async_copy(sources[i], targets[i], vectors_arrived.at[i]) for i in range(fetched)]
    for fetch in fetches:
        fetch.start()
    acc = jnp.zeros((8, channels), F32)
    for f in range(frames):
        for r in range(rows):
            copies[f][r].wait()
            acc = acc + jnp.sum(own_ref[f, r].astype(F32).reshape(width // 8, 8, channels), axis=0)
    channel_sum = jnp.broadcast_to(jnp.sum(acc, axis=0, keepdims=True), (8, channels))
    mean = channel_sum * (1.0 / count)
    acc = jnp.zeros((8, channels), F32)
    for f in range(frames):
        for r in range(rows):
            away = own_ref[f, r].astype(F32).reshape(width // 8, 8, channels) - mean[None]
            acc = acc + jnp.sum(away * away, axis=0)
    channel_square = jnp.broadcast_to(jnp.sum(acc, axis=0, keepdims=True), (8, channels))
    packed = pack_moments(channel_sum, channel_square, count)
    out_ref[...] = jnp.broadcast_to(packed, out_ref.shape)
    for fetch in fetches:
        fetch.wait()


PIECE = 64
PAD = 8


def position():
    core = lax.axis_index("rows_2")
    row_block = lax.axis_index(ROWS)
    last = lax.axis_size(ROWS) - 1
    inter_exists = jnp.where(core == 0, row_block > 0, row_block < last)
    frames_exist = lax.axis_index("tm") > 0
    return core, jnp.where(frames_exist, 1.0, 0.0).astype(F32), jnp.where(inter_exists, 1.0, 0.0).astype(F32)


def act_steps(f, act_ref, sources, place, scale, offset, bias):
    own_ref, prior_ref, inter_ref, intra_ref = sources
    core, frames_exist, inter_exists = place
    width = own_ref.shape[2]
    half = PIECE // 2
    source = prior_ref.at[f] if f < 2 else own_ref.at[f - 2]
    keep = frames_exist if f < 2 else None
    inter_keep = inter_exists if keep is None else keep * inter_exists
    blocks = [
        (inter_ref.at[f], core * 3, inter_keep),
        (source.at[0], 1, keep),
        (source.at[1], 2, keep),
        (intra_ref.at[f], 3 - core * 3, keep),
    ]

    def step(block, at):
        cells, row, keep = block
        v = cells[at : at + half].astype(F32)
        if bias is not None:
            v = v + bias
        h = v * scale + offset
        silu = h + h * jnp.tanh(h)
        if keep is not None:
            silu = silu * keep
        act_ref[row, at : at + half] = silu.astype(BF16)

    return [functools.partial(step, block, at) for block in blocks for at in range(0, width, half)]


def conv_steps(act_ref, weight_ref, i, sums_ref, ready):
    width, channels = act_ref.shape[1], act_ref.shape[2]

    def step(k):
        ready(i, k)
        part = None
        for j in range(3):
            window = act_ref[j : j + 2].reshape(2 * width, channels)
            product = jnp.dot(window, weight_ref[i, j, k], preferred_element_type=F32)
            part = product if part is None else part + product
        for r in range(2):
            row = part[r * width : (r + 1) * width]
            if i > 0:
                row = row + sums_ref[k, r, PAD : PAD + width]
            sums_ref[k, r, PAD : PAD + width] = row

    return [functools.partial(step, k) for k in range(3)]


def clear_pads(sums_ref):
    width = sums_ref.shape[2] - 2 * PAD
    channels = sums_ref.shape[3]
    for r in range(2):
        sums_ref[0, r, 0:PAD] = jnp.zeros((PAD, channels), F32)
        sums_ref[2, r, PAD + width :] = jnp.zeros((PAD, channels), F32)


def piece_of(sums_ref, r, at):
    left = sums_ref[0, r, PAD + at - 1 : PAD + at - 1 + PIECE]
    middle = sums_ref[1, r, PAD + at : PAD + at + PIECE]
    right = sums_ref[2, r, PAD + at + 1 : PAD + at + 1 + PIECE]
    return middle + left + right


def beside(main, other):
    done = 0
    for n, step in enumerate(main):
        step()
        until = len(other) * (n + 1) // len(main)
        for extra in other[done:until]:
            extra()
        done = until


def run(steps):
    for step in steps:
        step()


def fetch_weights(weight_hbm, weight_ref, arrived):
    copies = {}
    for i in range(3):
        for k in range(3):
            copy = pltpu.make_async_copy(weight_hbm.at[i, :, k], weight_ref.at[i, :, k], arrived.at[i, k])
            copy.start()
            copies[i, k] = copy

    def ready(i, k):
        if (i, k) in copies:
            copies.pop((i, k)).wait()

    return ready


def first_kernel(
    prior_ref, inter_ref, intra_ref, gathered_ref, gain_ref, shift_ref, bias_ref, latents_hbm, weight_hbm,
    hidden_ref, moments_ref, *scratch, count,
):
    acts, sums, (weight_ref, arrived, own_ref, own_arrived) = scratch[:4], scratch[4:6], scratch[6:]
    width, channels = own_ref.shape[2], own_ref.shape[3]
    ready = fetch_weights(weight_hbm, weight_ref, arrived)
    fetch_own = pltpu.make_async_copy(latents_hbm, own_ref, own_arrived)
    fetch_own.start()
    for ref in sums:
        clear_pads(ref)
    scale, offset = merge_moments(gathered_ref[...], count, gain_ref[...], shift_ref[...], channels)
    place = position()
    sources = (own_ref, prior_ref, inter_ref, intra_ref)
    acting = [act_steps(f, acts[f], sources, place, scale, offset, None) for f in range(4)]
    totals = {}

    def finish(t, r, at):
        piece = piece_of(sums[t], r, at)
        hidden_ref[t, r, at : at + PIECE] = piece.astype(BF16)
        if not totals:
            totals["pivot"] = jnp.sum(piece, axis=0, keepdims=True) * (1.0 / PIECE)
            totals["sum"] = jnp.zeros((8, channels), F32)
            totals["square"] = jnp.zeros((8, channels), F32)
        away = (piece - totals["pivot"]).reshape(PIECE // 8, 8, channels)
        totals["sum"] = totals["sum"] + jnp.sum(away, axis=0)
        totals["square"] = totals["square"] + jnp.sum(away * away, axis=0)

    def finishing(t):
        return [functools.partial(finish, t, r, at) for r in range(2) for at in range(0, width, PIECE)]

    taps = lambda f, t: conv_steps(acts[f], weight_ref, f - t, sums[t], ready)
    run(acting[0])
    beside(taps(0, 0), acting[1])
    fetch_own.wait()
    beside(taps(1, 0) + taps(1, 1), acting[2])
    beside(taps(2, 0) + taps(2, 1), acting[3])
    beside(taps(3, 1), finishing(0))
    run(finishing(1))

    cells = 4.0 * width
    away = jnp.broadcast_to(jnp.sum(totals["sum"], axis=0, keepdims=True), (8, channels))
    square = jnp.broadcast_to(jnp.sum(totals["square"], axis=0, keepdims=True), (8, channels))
    square = jnp.maximum(square - away * away * (1.0 / cells), 0.0)
    total = away + cells * (totals["pivot"] + bias_ref[...])
    moments_ref[...] = jnp.broadcast_to(pack_moments(total, square, cells), moments_ref.shape)


def second_kernel(
    own_ref, prior_ref, inter_ref, intra_ref, gathered_ref, gain_ref, shift_ref, bias1_ref, bias2_ref, up_bias_ref,
    latents_hbm, weight_hbm, up_hbm, video_ref, *scratch, count,
):
    acts, sums = scratch[:4], scratch[4:6]
    wide_ref, block_ref, stage_ref, sent, weight_ref, arrived, latents_ref, up_ref, other_arrived = scratch[6:]
    width, channels = own_ref.shape[2], own_ref.shape[3]
    ready = fetch_weights(weight_hbm, weight_ref, arrived)
    fetch_latents = pltpu.make_async_copy(latents_hbm, latents_ref, other_arrived.at[0])
    fetch_latents.start()
    fetch_up = pltpu.make_async_copy(up_hbm, up_ref, other_arrived.at[1])
    fetch_up.start()
    for ref in sums:
        clear_pads(ref)
    scale, offset = merge_moments(gathered_ref[...], count, gain_ref[...], shift_ref[...], channels)
    place = position()
    sources = (own_ref, prior_ref, inter_ref, intra_ref)
    acting = [act_steps(f, acts[f], sources, place, scale, offset, bias1_ref[...]) for f in range(4)]

    def sending(t, a, b, r):
        return pltpu.make_async_copy(
            stage_ref.at[t, a, 2 * r + b], video_ref.at[2 * t + a, 2 * r + b], sent.at[t, a, 2 * r + b]
        )

    def finish(t, r, at):
        latents = latents_ref[t, r, at : at + PIECE].astype(F32)
        block = latents + (piece_of(sums[t], r, at) + bias2_ref[...])
        block_ref[t, r * width + at : r * width + at + PIECE] = block.astype(BF16)

    def finishing(t):
        return [functools.partial(finish, t, r, at) for r in range(2) for at in range(0, width, PIECE)]

    def widen(t, a, b, e):
        n = ((2 * a + b) * 2 + e) * channels
        part = jnp.dot(block_ref[t], up_ref[:, n : n + channels], preferred_element_type=F32)
        part = part + up_bias_ref[:, n : n + channels]
        for lane in range(0, channels, LANES):
            wide_ref[2 * a + b, lane // LANES, pl.ds(e, 2 * width, stride=2), :] = part[:, lane : lane + LANES]

    def send(t, a, b):
        for r in range(2):
            for lane in range(0, channels, LANES):
                stage_ref[t, a, 2 * r + b, :, lane : lane + LANES] = wide_ref[
                    2 * a + b, lane // LANES, 2 * width * r : 2 * width * (r + 1), :
                ].astype(BF16)
            sending(t, a, b, r).start()

    def widening(t):
        steps = []
        for a in range(2):
            for b in range(2):
                steps += [functools.partial(widen, t, a, b, e) for e in range(2)]
                steps.append(functools.partial(send, t, a, b))
        return steps

    taps = lambda f, t: conv_steps(acts[f], weight_ref, f - t, sums[t], ready)
    run(acting[0])
    beside(taps(0, 0), acting[1])
    beside(taps(1, 0) + taps(1, 1), acting[2])
    run(taps(2, 0))
    fetch_latents.wait()
    beside(taps(2, 1), acting[3] + finishing(0))
    fetch_up.wait()
    beside(taps(3, 1), widening(0))
    run(finishing(1))
    run(widening(1))
    for t in range(2):
        for a in range(2):
            for b in range(2):
                for r in range(2):
                    sending(t, a, b, r).wait()


def edges_kernel(own_ref, prior_ref, outward_ref, inward_ref):
    core = lax.axis_index("rows_2")
    for f in range(4):
        source = prior_ref.at[f] if f < 2 else own_ref.at[f - 2]
        outward_ref[f] = source[core]
        inward_ref[f] = source[1 - core]


VMEM = pl.BlockSpec(memory_space=pltpu.MemorySpace.VMEM)
HBM = pl.BlockSpec(memory_space=pltpu.MemorySpace.HBM)


def in_hbm(x):
    return pltpu.with_memory_space_constraint(x, pltpu.MemorySpace.HBM)


def params(mebibytes):
    return pltpu.CompilerParams(
        vmem_limit_bytes=mebibytes * 1024 * 1024
    )


def send_on(cells):
    return lax.ppermute(cells, "tm", [(i, i + 1) for i in range(lax.axis_size("tm") - 1)])


FIRST = ROWS
SECOND = "tm"


def share(moments, axes):
    return lax.all_to_all(moments, axes, split_axis=0, concat_axis=0, tiled=True)


def share_all(moments, count):
    first = share(moments, FIRST)
    merged = pl.pallas_call(
        functools.partial(merge_kernel, count=count),
        in_specs=[VMEM],
        out_specs=VMEM,
        out_shape=jax.ShapeDtypeStruct((lax.axis_size(SECOND), LANES), F32),
        compiler_params=pltpu.CompilerParams(vmem_limit_bytes=1024 * 1024),
    )(first)
    return share(merged, SECOND)


def send_edges(cells, prior):
    frames, _, width, channels = cells.shape
    edge = jax.ShapeDtypeStruct((2 * frames, width, channels), BF16)
    outward, inward = pl.pallas_call(
        edges_kernel,
        in_specs=[VMEM, VMEM],
        out_specs=[VMEM, VMEM],
        out_shape=[edge, edge],
        compiler_params=pltpu.CompilerParams(vmem_limit_bytes=1024 * 1024),
    )(cells, prior)
    rows = lax.axis_size(ROWS)
    between = [(i, i + 1) for i in range(1, rows - 1, 2)] + [(i + 1, i) for i in range(1, rows - 1, 2)]
    within = [(i, i ^ 1) for i in range(rows)]
    inter = lax.ppermute(outward, ROWS, between)
    intra = lax.ppermute(inward, ROWS, within)
    return inter, intra


def body(
    latents,
    norm1_gain,
    norm1_shift,
    conv1_weight,
    conv1_bias,
    norm2_gain,
    norm2_shift,
    conv2_weight,
    conv2_bias,
    up_weight,
    up_bias,
):
    frames, rows, width, channels = latents.shape
    moments_shape = jax.ShapeDtypeStruct((lax.axis_size(FIRST), LANES), F32)
    cells_shape = jax.ShapeDtypeStruct(latents.shape, BF16)
    acts = [pltpu.VMEM((rows + 2, width, channels), BF16)] * (2 * frames)
    sums = [pltpu.VMEM((3, rows, width + 2 * PAD, channels), F32)] * frames
    one_device = frames * rows * width * (channels // GROUPS)
    one_row = one_device * lax.axis_size(FIRST)
    vectors = (norm1_gain, norm1_shift, conv1_bias, norm2_gain, norm2_shift, conv2_bias, up_bias)
    vectors = [v.reshape(1, -1) for v in vectors]

    moments, own, gain1, shift1, bias1, gain2, shift2, bias2, bias_up = pl.pallas_call(
        stats_kernel,
        in_specs=[HBM] * (1 + len(vectors)),
        out_specs=[VMEM] * (2 + len(vectors)),
        out_shape=[moments_shape, cells_shape] + [jax.ShapeDtypeStruct(v.shape, F32) for v in vectors],
        scratch_shapes=[
            pltpu.SemaphoreType.DMA((frames, rows)),
            pltpu.SemaphoreType.DMA((len(vectors),)),
        ],
        compiler_params=pltpu.CompilerParams(vmem_limit_bytes=1024 * 1024),
    )(*map(in_hbm, (latents, *vectors)))
    prior = send_on(own)
    inter, intra = send_edges(own, prior)
    gathered = share_all(moments, one_device)
    hidden, moments = pl.pallas_call(
        functools.partial(first_kernel, count=one_row),
        in_specs=[VMEM] * 7 + [HBM] * 2,
        out_specs=[VMEM, VMEM],
        out_shape=[cells_shape, moments_shape],
        scratch_shapes=[
            *acts,
            *sums,
            pltpu.VMEM(conv1_weight.shape, BF16),
            pltpu.SemaphoreType.DMA((3, 3)),
            pltpu.VMEM(latents.shape, BF16),
            pltpu.SemaphoreType.DMA(()),
        ],
        compiler_params=params(20),
    )(prior, inter, intra, gathered, gain1, shift1, bias1, in_hbm(latents), in_hbm(conv1_weight))

    prior = send_on(hidden)
    inter, intra = send_edges(hidden, prior)
    gathered = share_all(moments, one_device)
    return pl.pallas_call(
        functools.partial(second_kernel, count=one_row),
        in_specs=[VMEM] * 10 + [HBM] * 3,
        out_specs=HBM,
        out_shape=jax.ShapeDtypeStruct((2 * frames, 2 * rows, 2 * width, channels), BF16),
        scratch_shapes=[
            *acts,
            *sums,
            pltpu.VMEM((4, channels // LANES, 2 * rows * width, LANES), F32),
            pltpu.VMEM((frames, rows * width, channels), BF16),
            pltpu.VMEM((frames, 2, 2 * rows, 2 * width, channels), BF16),
            pltpu.SemaphoreType.DMA((frames, 2, 2 * rows)),
            pltpu.VMEM(conv2_weight.shape, BF16),
            pltpu.SemaphoreType.DMA((3, 3)),
            pltpu.VMEM(latents.shape, BF16),
            pltpu.VMEM(up_weight.shape, BF16),
            pltpu.SemaphoreType.DMA((2,)),
        ],
        compiler_params=params(32),
    )(
        hidden, prior, inter, intra, gathered, gain2, shift2, bias1, bias2, bias_up,
        in_hbm(latents), in_hbm(conv2_weight), in_hbm(up_weight),
    )


def solution(mesh):
    finer = Mesh(
        mesh.devices.reshape(mesh.shape["tm"], 8, 4, 2), ("tm", "rows_0", "rows_1", "rows_2")
    )
    placed = (P("tm", ROWS, None, None), P(), P(), P(), P(), P(), P(), P(), P(), P(), P())
    return jax.shard_map(
        body, mesh=finer, in_specs=placed, out_specs=P("tm", ROWS, None, None), check_vma=False
    )
```

```python
import functools

import jax
import jax.numpy as jnp
from jax import lax
from jax.experimental import pallas as pl
from jax.experimental.pallas import tpu as pltpu
from jax.sharding import Mesh
from jax.sharding import PartitionSpec as P


GROUPS = 32
EPSILON = 1e-06
ROWS = ("rows_0", "rows_1", "rows_2")
F32 = jnp.float32
BF16 = jnp.bfloat16
LANES = 128


def split_rows(first, second):
    row = lax.broadcasted_iota(jnp.int32, first.shape, 0)
    value = jnp.where(row < 3, first, second)
    high = value.astype(BF16).astype(F32)
    middle = (value - high).astype(BF16).astype(F32)
    low = value - high - middle
    step = jnp.where(row < 3, row, row - 3)
    part = jnp.where(step == 0, high, jnp.where(step == 1, middle, low))
    return jnp.where(row < 6, part, 0.0).astype(BF16)


def joined_rows(product):
    row = lax.broadcasted_iota(jnp.int32, product.shape, 0)
    first = jnp.sum(jnp.where(row < 3, product, 0.0), axis=0, keepdims=True)
    second = jnp.sum(jnp.where((row >= 3) & (row < 6), product, 0.0), axis=0, keepdims=True)
    return first, second


def group_sum(value, per_group):
    lane = lax.broadcasted_iota(jnp.int32, value.shape, 1)
    channels = value.shape[1]
    step = 1
    while step < per_group:
        other = jnp.where(lane & step == 0, pltpu.roll(value, channels - step, 1), pltpu.roll(value, step, 1))
        value = value + other
        step *= 2
    return value


def pack_moments(channel_sum, channel_square, count):
    channels = channel_sum.shape[1]
    per_group = channels // GROUPS
    channel_mean = channel_sum * (1.0 / count)
    group_mean = group_sum(channel_mean, per_group) * (1.0 / per_group)
    spread = channel_mean - group_mean
    square = channel_square + spread * spread * count
    lane = lax.broadcasted_iota(jnp.int32, (channels, LANES), 1)
    group = lax.broadcasted_iota(jnp.int32, (channels, LANES), 0) // per_group
    chosen = ((lane == group) | (lane == group + GROUPS)).astype(F32).astype(BF16)
    product = jnp.dot(split_rows(channel_mean * (1.0 / per_group), square), chosen, preferred_element_type=F32)
    mean, square = joined_rows(product)
    lane = lax.broadcasted_iota(jnp.int32, (1, LANES), 1)
    return jnp.where(lane < GROUPS, mean, square)


def merge_moments(gathered, count, gain, shift, channels):
    devices = gathered.shape[0]
    per_group = channels // GROUPS
    total = jnp.broadcast_to(jnp.sum(gathered, axis=0, keepdims=True), (8, LANES))
    away = gathered - (total * (1.0 / devices))[0:1]
    between = jnp.broadcast_to(jnp.sum(away * away, axis=0, keepdims=True), (8, LANES))
    lane = lax.broadcasted_iota(jnp.int32, (LANES, 2 * channels), 0)
    column = lax.broadcasted_iota(jnp.int32, (LANES, 2 * channels), 1)
    chosen = (lane == column // per_group).astype(F32).astype(BF16)
    product = jnp.dot(split_rows(total, between), chosen, preferred_element_type=F32)
    first, second = joined_rows(product)
    mean = first[:, :channels] * (1.0 / devices)
    within = first[:, channels:]
    variance = (within + second[:, :channels] * count) * (1.0 / (count * devices))
    scale = gain / jnp.sqrt(variance + EPSILON)
    return 0.5 * scale, 0.5 * (shift - mean * scale)


def merge_kernel(gathered_ref, out_ref, *, count):
    gathered = gathered_ref[...]
    members = gathered.shape[0]
    total = jnp.sum(gathered, axis=0, keepdims=True)
    mean = total * (1.0 / members)
    away = gathered - mean
    between = jnp.broadcast_to(jnp.sum(away * away, axis=0, keepdims=True), (8, LANES))
    square = total + pltpu.roll(between, GROUPS, 1)[0:1] * count
    lane = lax.broadcasted_iota(jnp.int32, (1, LANES), 1)
    out_ref[...] = jnp.broadcast_to(jnp.where(lane < GROUPS, mean, square), out_ref.shape)


def stats_kernel(values_ref, *refs):
    fetched = (len(refs) - 4) // 2
    sources = refs[:fetched]
    out_ref, own_ref = refs[fetched : fetched + 2]
    targets = refs[fetched + 2 : 2 * fetched + 2]
    arrived, vectors_arrived = refs[2 * fetched + 2 :]
    frames, rows, width, channels = own_ref.shape
    count = frames * rows * width
    copies = [
        [pltpu.make_async_copy(values_ref.at[f, r], own_ref.at[f, r], arrived.at[f, r]) for r in range(rows)]
        for f in range(frames)
    ]
    for f in range(frames):
        for r in range(rows):
            copies[f][r].start()
    fetches = [pltpu.make_async_copy(sources[i], targets[i], vectors_arrived.at[i]) for i in range(fetched)]
    for fetch in fetches:
        fetch.start()
    acc = jnp.zeros((8, channels), F32)
    for f in range(frames):
        for r in range(rows):
            copies[f][r].wait()
            acc = acc + jnp.sum(own_ref[f, r].astype(F32).reshape(width // 8, 8, channels), axis=0)
    channel_sum = jnp.broadcast_to(jnp.sum(acc, axis=0, keepdims=True), (8, channels))
    mean = channel_sum * (1.0 / count)
    acc = jnp.zeros((8, channels), F32)
    for f in range(frames):
        for r in range(rows):
            away = own_ref[f, r].astype(F32).reshape(width // 8, 8, channels) - mean[None]
            acc = acc + jnp.sum(away * away, axis=0)
    channel_square = jnp.broadcast_to(jnp.sum(acc, axis=0, keepdims=True), (8, channels))
    packed = pack_moments(channel_sum, channel_square, count)
    out_ref[...] = jnp.broadcast_to(packed, out_ref.shape)
    for fetch in fetches:
        fetch.wait()


PIECE = 64
PAD = 8


def position():
    core = lax.axis_index("rows_2")
    row_block = lax.axis_index(ROWS)
    last = lax.axis_size(ROWS) - 1
    inter_exists = jnp.where(core == 0, row_block > 0, row_block < last)
    frames_exist = lax.axis_index("tm") > 0
    return core, jnp.where(frames_exist, 1.0, 0.0).astype(F32), jnp.where(inter_exists, 1.0, 0.0).astype(F32)


def act_steps(f, act_ref, sources, place, scale, offset, bias):
    own_ref, prior_ref, inter_ref, intra_ref = sources
    core, frames_exist, inter_exists = place
    width = own_ref.shape[2]
    half = PIECE // 2
    source = prior_ref.at[f] if f < 2 else own_ref.at[f - 2]
    keep = frames_exist if f < 2 else None
    inter_keep = inter_exists if keep is None else keep * inter_exists
    blocks = [
        (inter_ref.at[f], core * 3, inter_keep),
        (source.at[0], 1, keep),
        (source.at[1], 2, keep),
        (intra_ref.at[f], 3 - core * 3, keep),
    ]

    def step(block, at):
        cells, row, keep = block
        v = cells[at : at + half].astype(F32)
        if bias is not None:
            v = v + bias
        h = v * scale + offset
        silu = h + h * jnp.tanh(h)
        if keep is not None:
            silu = silu * keep
        act_ref[row, at : at + half] = silu.astype(BF16)

    return [functools.partial(step, block, at) for block in blocks for at in range(0, width, half)]


def conv_steps(act_ref, weight_ref, i, sums_ref):
    width, channels = act_ref.shape[1], act_ref.shape[2]

    def step(k):
        part = None
        for j in range(3):
            window = act_ref[j : j + 2].reshape(2 * width, channels)
            product = jnp.dot(window, weight_ref[i, j, k], preferred_element_type=F32)
            part = product if part is None else part + product
        for r in range(2):
            row = part[r * width : (r + 1) * width]
            if i > 0:
                row = row + sums_ref[k, r, PAD : PAD + width]
            sums_ref[k, r, PAD : PAD + width] = row

    return [functools.partial(step, k) for k in range(3)]


def clear_pads(sums_ref):
    width = sums_ref.shape[2] - 2 * PAD
    channels = sums_ref.shape[3]
    for r in range(2):
        sums_ref[0, r, 0:PAD] = jnp.zeros((PAD, channels), F32)
        sums_ref[2, r, PAD + width :] = jnp.zeros((PAD, channels), F32)


def piece_of(sums_ref, r, at):
    left = sums_ref[0, r, PAD + at - 1 : PAD + at - 1 + PIECE]
    middle = sums_ref[1, r, PAD + at : PAD + at + PIECE]
    right = sums_ref[2, r, PAD + at + 1 : PAD + at + 1 + PIECE]
    return middle + left + right


def beside(main, other):
    done = 0
    for n, step in enumerate(main):
        step()
        until = len(other) * (n + 1) // len(main)
        for extra in other[done:until]:
            extra()
        done = until


def run(steps):
    for step in steps:
        step()


def fetch_weights(weight_hbm, weight_ref, arrived):
    copies = [
        [pltpu.make_async_copy(weight_hbm.at[i, j], weight_ref.at[i, j], arrived.at[i, j]) for j in range(3)]
        for i in range(3)
    ]
    for part in copies:
        for copy in part:
            copy.start()

    def ready(i):
        for copy in copies[i]:
            copy.wait()

    return ready


def first_kernel(
    prior_ref, inter_ref, intra_ref, gathered_ref, gain_ref, shift_ref, bias_ref, latents_hbm, weight_hbm,
    hidden_ref, moments_ref, *scratch, count,
):
    acts, sums, (weight_ref, arrived, own_ref, own_arrived) = scratch[:4], scratch[4:6], scratch[6:]
    width, channels = own_ref.shape[2], own_ref.shape[3]
    ready = fetch_weights(weight_hbm, weight_ref, arrived)
    fetch_own = pltpu.make_async_copy(latents_hbm, own_ref, own_arrived)
    fetch_own.start()
    for ref in sums:
        clear_pads(ref)
    scale, offset = merge_moments(gathered_ref[...], count, gain_ref[...], shift_ref[...], channels)
    place = position()
    sources = (own_ref, prior_ref, inter_ref, intra_ref)
    acting = [act_steps(f, acts[f], sources, place, scale, offset, None) for f in range(4)]
    totals = {}

    def finish(t, r, at):
        piece = piece_of(sums[t], r, at)
        hidden_ref[t, r, at : at + PIECE] = piece.astype(BF16)
        if not totals:
            totals["pivot"] = jnp.sum(piece, axis=0, keepdims=True) * (1.0 / PIECE)
            totals["sum"] = jnp.zeros((8, channels), F32)
            totals["square"] = jnp.zeros((8, channels), F32)
        away = (piece - totals["pivot"]).reshape(PIECE // 8, 8, channels)
        totals["sum"] = totals["sum"] + jnp.sum(away, axis=0)
        totals["square"] = totals["square"] + jnp.sum(away * away, axis=0)

    def finishing(t):
        return [functools.partial(finish, t, r, at) for r in range(2) for at in range(0, width, PIECE)]

    taps = lambda f, t: conv_steps(acts[f], weight_ref, f - t, sums[t])
    run(acting[0] + acting[1])
    ready(0)
    run(taps(0, 0))
    ready(1)
    ready(2)
    fetch_own.wait()
    beside(taps(1, 0) + taps(1, 1), acting[2])
    beside(taps(2, 0) + taps(2, 1), acting[3])
    beside(taps(3, 1), finishing(0))
    run(finishing(1))

    cells = 4.0 * width
    away = jnp.broadcast_to(jnp.sum(totals["sum"], axis=0, keepdims=True), (8, channels))
    square = jnp.broadcast_to(jnp.sum(totals["square"], axis=0, keepdims=True), (8, channels))
    square = jnp.maximum(square - away * away * (1.0 / cells), 0.0)
    total = away + cells * (totals["pivot"] + bias_ref[...])
    moments_ref[...] = jnp.broadcast_to(pack_moments(total, square, cells), moments_ref.shape)


def second_kernel(
    own_ref, prior_ref, inter_ref, intra_ref, gathered_ref, gain_ref, shift_ref, bias1_ref, bias2_ref, up_bias_ref,
    latents_hbm, weight_hbm, up_hbm, video_ref, *scratch, count,
):
    acts, sums = scratch[:4], scratch[4:6]
    wide_ref, block_ref, stage_ref, sent, weight_ref, arrived, latents_ref, up_ref, other_arrived = scratch[6:]
    width, channels = own_ref.shape[2], own_ref.shape[3]
    ready = fetch_weights(weight_hbm, weight_ref, arrived)
    fetch_latents = pltpu.make_async_copy(latents_hbm, latents_ref, other_arrived.at[0])
    fetch_latents.start()
    fetch_up = pltpu.make_async_copy(up_hbm, up_ref, other_arrived.at[1])
    fetch_up.start()
    for ref in sums:
        clear_pads(ref)
    scale, offset = merge_moments(gathered_ref[...], count, gain_ref[...], shift_ref[...], channels)
    place = position()
    sources = (own_ref, prior_ref, inter_ref, intra_ref)
    acting = [act_steps(f, acts[f], sources, place, scale, offset, bias1_ref[...]) for f in range(4)]

    def sending(t, a, b, r):
        return pltpu.make_async_copy(
            stage_ref.at[t, a, 2 * r + b], video_ref.at[2 * t + a, 2 * r + b], sent.at[t, a, 2 * r + b]
        )

    def finish(t, r, at):
        latents = latents_ref[t, r, at : at + PIECE].astype(F32)
        block = latents + (piece_of(sums[t], r, at) + bias2_ref[...])
        block_ref[t, r * width + at : r * width + at + PIECE] = block.astype(BF16)

    def finishing(t):
        return [functools.partial(finish, t, r, at) for r in range(2) for at in range(0, width, PIECE)]

    def widen(t, a, b, e):
        n = ((2 * a + b) * 2 + e) * channels
        part = jnp.dot(block_ref[t], up_ref[:, n : n + channels], preferred_element_type=F32)
        part = part + up_bias_ref[:, n : n + channels]
        for lane in range(0, channels, LANES):
            wide_ref[2 * a + b, lane // LANES, pl.ds(e, 2 * width, stride=2), :] = part[:, lane : lane + LANES]

    def send(t, a, b):
        for r in range(2):
            for lane in range(0, channels, LANES):
                stage_ref[t, a, 2 * r + b, :, lane : lane + LANES] = wide_ref[
                    2 * a + b, lane // LANES, 2 * width * r : 2 * width * (r + 1), :
                ].astype(BF16)
            sending(t, a, b, r).start()

    def widening(t):
        steps = []
        for a in range(2):
            for b in range(2):
                steps += [functools.partial(widen, t, a, b, e) for e in range(2)]
                steps.append(functools.partial(send, t, a, b))
        return steps

    taps = lambda f, t: conv_steps(acts[f], weight_ref, f - t, sums[t])
    run(acting[0] + acting[1])
    ready(0)
    beside(taps(0, 0), acting[2])
    ready(1)
    ready(2)
    fetch_latents.wait()
    beside(taps(1, 0) + taps(1, 1), acting[3])
    run(taps(2, 0))
    beside(taps(2, 1), finishing(0))
    fetch_up.wait()
    beside(taps(3, 1), widening(0))
    run(finishing(1))
    run(widening(1))
    for t in range(2):
        for a in range(2):
            for b in range(2):
                for r in range(2):
                    sending(t, a, b, r).wait()


def edges_kernel(own_ref, prior_ref, outward_ref, inward_ref):
    core = lax.axis_index("rows_2")
    for f in range(4):
        source = prior_ref.at[f] if f < 2 else own_ref.at[f - 2]
        outward_ref[f] = source[core]
        inward_ref[f] = source[1 - core]


VMEM = pl.BlockSpec(memory_space=pltpu.MemorySpace.VMEM)
HBM = pl.BlockSpec(memory_space=pltpu.MemorySpace.HBM)


def in_hbm(x):
    return pltpu.with_memory_space_constraint(x, pltpu.MemorySpace.HBM)


def params(mebibytes):
    return pltpu.CompilerParams(
        vmem_limit_bytes=mebibytes * 1024 * 1024
    )


def send_on(cells):
    return lax.ppermute(cells, "tm", [(i, i + 1) for i in range(lax.axis_size("tm") - 1)])


FIRST = ROWS
SECOND = "tm"


def share(moments, axes):
    return lax.all_to_all(moments, axes, split_axis=0, concat_axis=0, tiled=True)


def share_all(moments, count):
    first = share(moments, FIRST)
    merged = pl.pallas_call(
        functools.partial(merge_kernel, count=count),
        in_specs=[VMEM],
        out_specs=VMEM,
        out_shape=jax.ShapeDtypeStruct((lax.axis_size(SECOND), LANES), F32),
        compiler_params=pltpu.CompilerParams(vmem_limit_bytes=1024 * 1024),
    )(first)
    return share(merged, SECOND)


def send_edges(cells, prior):
    frames, _, width, channels = cells.shape
    edge = jax.ShapeDtypeStruct((2 * frames, width, channels), BF16)
    outward, inward = pl.pallas_call(
        edges_kernel,
        in_specs=[VMEM, VMEM],
        out_specs=[VMEM, VMEM],
        out_shape=[edge, edge],
        compiler_params=pltpu.CompilerParams(vmem_limit_bytes=1024 * 1024),
    )(cells, prior)
    rows = lax.axis_size(ROWS)
    between = [(i, i + 1) for i in range(1, rows - 1, 2)] + [(i + 1, i) for i in range(1, rows - 1, 2)]
    within = [(i, i ^ 1) for i in range(rows)]
    inter = lax.ppermute(outward, ROWS, between)
    intra = lax.ppermute(inward, ROWS, within)
    return inter, intra


def body(
    latents,
    norm1_gain,
    norm1_shift,
    conv1_weight,
    conv1_bias,
    norm2_gain,
    norm2_shift,
    conv2_weight,
    conv2_bias,
    up_weight,
    up_bias,
):
    frames, rows, width, channels = latents.shape
    moments_shape = jax.ShapeDtypeStruct((lax.axis_size(FIRST), LANES), F32)
    cells_shape = jax.ShapeDtypeStruct(latents.shape, BF16)
    acts = [pltpu.VMEM((rows + 2, width, channels), BF16)] * (2 * frames)
    sums = [pltpu.VMEM((3, rows, width + 2 * PAD, channels), F32)] * frames
    one_device = frames * rows * width * (channels // GROUPS)
    one_row = one_device * lax.axis_size(FIRST)
    vectors = (norm1_gain, norm1_shift, conv1_bias, norm2_gain, norm2_shift, conv2_bias, up_bias)
    vectors = [v.reshape(1, -1) for v in vectors]

    prior = send_on(latents)
    moments, own, gain1, shift1, bias1, gain2, shift2, bias2, bias_up = pl.pallas_call(
        stats_kernel,
        in_specs=[HBM] * (1 + len(vectors)),
        out_specs=[VMEM] * (2 + len(vectors)),
        out_shape=[moments_shape, cells_shape] + [jax.ShapeDtypeStruct(v.shape, F32) for v in vectors],
        scratch_shapes=[
            pltpu.SemaphoreType.DMA((frames, rows)),
            pltpu.SemaphoreType.DMA((len(vectors),)),
        ],
        compiler_params=pltpu.CompilerParams(vmem_limit_bytes=1024 * 1024),
    )(*map(in_hbm, (latents, *vectors)))
    inter, intra = send_edges(own, prior)
    gathered = share_all(moments, one_device)
    hidden, moments = pl.pallas_call(
        functools.partial(first_kernel, count=one_row),
        in_specs=[VMEM] * 7 + [HBM] * 2,
        out_specs=[VMEM, VMEM],
        out_shape=[cells_shape, moments_shape],
        scratch_shapes=[
            *acts,
            *sums,
            pltpu.VMEM(conv1_weight.shape, BF16),
            pltpu.SemaphoreType.DMA((3, 3)),
            pltpu.VMEM(latents.shape, BF16),
            pltpu.SemaphoreType.DMA(()),
        ],
        compiler_params=params(20),
    )(prior, inter, intra, gathered, gain1, shift1, bias1, in_hbm(latents), in_hbm(conv1_weight))

    prior = send_on(hidden)
    inter, intra = send_edges(hidden, prior)
    gathered = share_all(moments, one_device)
    return pl.pallas_call(
        functools.partial(second_kernel, count=one_row),
        in_specs=[VMEM] * 10 + [HBM] * 3,
        out_specs=HBM,
        out_shape=jax.ShapeDtypeStruct((2 * frames, 2 * rows, 2 * width, channels), BF16),
        scratch_shapes=[
            *acts,
            *sums,
            pltpu.VMEM((4, channels // LANES, 2 * rows * width, LANES), F32),
            pltpu.VMEM((frames, rows * width, channels), BF16),
            pltpu.VMEM((frames, 2, 2 * rows, 2 * width, channels), BF16),
            pltpu.SemaphoreType.DMA((frames, 2, 2 * rows)),
            pltpu.VMEM(conv2_weight.shape, BF16),
            pltpu.SemaphoreType.DMA((3, 3)),
            pltpu.VMEM(latents.shape, BF16),
            pltpu.VMEM(up_weight.shape, BF16),
            pltpu.SemaphoreType.DMA((2,)),
        ],
        compiler_params=params(32),
    )(
        hidden, prior, inter, intra, gathered, gain2, shift2, bias1, bias2, bias_up,
        in_hbm(latents), in_hbm(conv2_weight), in_hbm(up_weight),
    )


def solution(mesh):
    finer = Mesh(
        mesh.devices.reshape(mesh.shape["tm"], 8, 4, 2), ("tm", "rows_0", "rows_1", "rows_2")
    )
    placed = (P("tm", ROWS, None, None), P(), P(), P(), P(), P(), P(), P(), P(), P(), P())
    return jax.shard_map(
        body, mesh=finer, in_specs=placed, out_specs=P("tm", ROWS, None, None), check_vma=False
    )
```

```python
import functools

import jax
import jax.numpy as jnp
from jax import lax
from jax.experimental import pallas as pl
from jax.experimental.pallas import tpu as pltpu
from jax.sharding import Mesh
from jax.sharding import PartitionSpec as P


GROUPS = 32
EPSILON = 1e-06
ROWS = ("rows_0", "rows_1", "rows_2")
F32 = jnp.float32
BF16 = jnp.bfloat16
LANES = 128


def split_rows(first, second):
    row = lax.broadcasted_iota(jnp.int32, first.shape, 0)
    value = jnp.where(row < 3, first, second)
    high = value.astype(BF16).astype(F32)
    middle = (value - high).astype(BF16).astype(F32)
    low = value - high - middle
    step = jnp.where(row < 3, row, row - 3)
    part = jnp.where(step == 0, high, jnp.where(step == 1, middle, low))
    return jnp.where(row < 6, part, 0.0).astype(BF16)


def joined_rows(product):
    row = lax.broadcasted_iota(jnp.int32, product.shape, 0)
    first = jnp.sum(jnp.where(row < 3, product, 0.0), axis=0, keepdims=True)
    second = jnp.sum(jnp.where((row >= 3) & (row < 6), product, 0.0), axis=0, keepdims=True)
    return first, second


def group_sum(value, per_group):
    lane = lax.broadcasted_iota(jnp.int32, value.shape, 1)
    channels = value.shape[1]
    step = 1
    while step < per_group:
        other = jnp.where(lane & step == 0, pltpu.roll(value, channels - step, 1), pltpu.roll(value, step, 1))
        value = value + other
        step *= 2
    return value


def pack_moments(channel_sum, channel_square, count):
    channels = channel_sum.shape[1]
    per_group = channels // GROUPS
    channel_mean = channel_sum * (1.0 / count)
    group_mean = group_sum(channel_mean, per_group) * (1.0 / per_group)
    spread = channel_mean - group_mean
    square = channel_square + spread * spread * count
    lane = lax.broadcasted_iota(jnp.int32, (channels, LANES), 1)
    group = lax.broadcasted_iota(jnp.int32, (channels, LANES), 0) // per_group
    chosen = ((lane == group) | (lane == group + GROUPS)).astype(F32).astype(BF16)
    product = jnp.dot(split_rows(channel_mean * (1.0 / per_group), square), chosen, preferred_element_type=F32)
    mean, square = joined_rows(product)
    lane = lax.broadcasted_iota(jnp.int32, (1, LANES), 1)
    return jnp.where(lane < GROUPS, mean, square)


def merge_moments(gathered, count, gain, shift, channels):
    devices = gathered.shape[0]
    per_group = channels // GROUPS
    total = jnp.broadcast_to(jnp.sum(gathered, axis=0, keepdims=True), (8, LANES))
    away = gathered - (total * (1.0 / devices))[0:1]
    between = jnp.broadcast_to(jnp.sum(away * away, axis=0, keepdims=True), (8, LANES))
    lane = lax.broadcasted_iota(jnp.int32, (LANES, 2 * channels), 0)
    column = lax.broadcasted_iota(jnp.int32, (LANES, 2 * channels), 1)
    chosen = (lane == column // per_group).astype(F32).astype(BF16)
    product = jnp.dot(split_rows(total, between), chosen, preferred_element_type=F32)
    first, second = joined_rows(product)
    mean = first[:, :channels] * (1.0 / devices)
    within = first[:, channels:]
    variance = (within + second[:, :channels] * count) * (1.0 / (count * devices))
    scale = gain / jnp.sqrt(variance + EPSILON)
    return 0.5 * scale, 0.5 * (shift - mean * scale)


def merge_kernel(gathered_ref, out_ref, *, count):
    gathered = gathered_ref[...]
    members = gathered.shape[0]
    total = jnp.sum(gathered, axis=0, keepdims=True)
    mean = total * (1.0 / members)
    away = gathered - mean
    between = jnp.broadcast_to(jnp.sum(away * away, axis=0, keepdims=True), (8, LANES))
    square = total + pltpu.roll(between, GROUPS, 1)[0:1] * count
    lane = lax.broadcasted_iota(jnp.int32, (1, LANES), 1)
    out_ref[...] = jnp.broadcast_to(jnp.where(lane < GROUPS, mean, square), out_ref.shape)


def stats_kernel(values_ref, *refs):
    fetched = (len(refs) - 4) // 2
    sources = refs[:fetched]
    out_ref, own_ref = refs[fetched : fetched + 2]
    targets = refs[fetched + 2 : 2 * fetched + 2]
    arrived, vectors_arrived = refs[2 * fetched + 2 :]
    frames, rows, width, channels = own_ref.shape
    count = frames * rows * width
    copies = [
        [pltpu.make_async_copy(values_ref.at[f, r], own_ref.at[f, r], arrived.at[f, r]) for r in range(rows)]
        for f in range(frames)
    ]
    for f in range(frames):
        for r in range(rows):
            copies[f][r].start()
    fetches = [pltpu.make_async_copy(sources[i], targets[i], vectors_arrived.at[i]) for i in range(fetched)]
    for fetch in fetches:
        fetch.start()
    acc = jnp.zeros((8, channels), F32)
    for f in range(frames):
        for r in range(rows):
            copies[f][r].wait()
            acc = acc + jnp.sum(own_ref[f, r].astype(F32).reshape(width // 8, 8, channels), axis=0)
    channel_sum = jnp.broadcast_to(jnp.sum(acc, axis=0, keepdims=True), (8, channels))
    mean = channel_sum * (1.0 / count)
    acc = jnp.zeros((8, channels), F32)
    for f in range(frames):
        for r in range(rows):
            away = own_ref[f, r].astype(F32).reshape(width // 8, 8, channels) - mean[None]
            acc = acc + jnp.sum(away * away, axis=0)
    channel_square = jnp.broadcast_to(jnp.sum(acc, axis=0, keepdims=True), (8, channels))
    packed = pack_moments(channel_sum, channel_square, count)
    out_ref[...] = jnp.broadcast_to(packed, out_ref.shape)
    for fetch in fetches:
        fetch.wait()


PIECE = 64
PAD = 8


def position():
    core = lax.axis_index("rows_2")
    row_block = lax.axis_index(ROWS)
    last = lax.axis_size(ROWS) - 1
    inter_exists = jnp.where(core == 0, row_block > 0, row_block < last)
    frames_exist = lax.axis_index("tm") > 0
    return core, jnp.where(frames_exist, 1.0, 0.0).astype(F32), jnp.where(inter_exists, 1.0, 0.0).astype(F32)


def act_steps(f, act_ref, sources, place, scale, offset):
    own_ref, prior_ref, inter_ref, intra_ref = sources
    core, frames_exist, inter_exists = place
    width = own_ref.shape[2]
    half = PIECE // 2
    source = prior_ref.at[f] if f < 2 else own_ref.at[f - 2]
    keep = frames_exist if f < 2 else None
    inter_keep = inter_exists if keep is None else keep * inter_exists
    blocks = [
        (inter_ref.at[f], core * 3, inter_keep),
        (source.at[0], 1, keep),
        (source.at[1], 2, keep),
        (intra_ref.at[f], 3 - core * 3, keep),
    ]

    def step(block, at):
        cells, row, keep = block
        v = cells[at : at + half].astype(F32)
        h = v * scale + offset
        silu = h + h * jnp.tanh(h)
        if keep is not None:
            silu = silu * keep
        act_ref[row, at : at + half] = silu.astype(BF16)

    return [functools.partial(step, block, at) for block in blocks for at in range(0, width, half)]


def conv_steps(act_ref, weight_ref, i, sums_ref):
    width, channels = act_ref.shape[1], act_ref.shape[2]

    def step(k):
        part = None
        for j in range(3):
            window = act_ref[j : j + 2].reshape(2 * width, channels)
            product = jnp.dot(window, weight_ref[i, j, k], preferred_element_type=F32)
            part = product if part is None else part + product
        for r in range(2):
            row = part[r * width : (r + 1) * width]
            if i > 0:
                row = row + sums_ref[k, r, PAD : PAD + width]
            sums_ref[k, r, PAD : PAD + width] = row

    return [functools.partial(step, k) for k in range(3)]


def clear_pads(sums_ref):
    width = sums_ref.shape[2] - 2 * PAD
    channels = sums_ref.shape[3]
    for r in range(2):
        sums_ref[0, r, 0:PAD] = jnp.zeros((PAD, channels), F32)
        sums_ref[2, r, PAD + width :] = jnp.zeros((PAD, channels), F32)


def piece_of(sums_ref, r, at):
    left = sums_ref[0, r, PAD + at - 1 : PAD + at - 1 + PIECE]
    middle = sums_ref[1, r, PAD + at : PAD + at + PIECE]
    right = sums_ref[2, r, PAD + at + 1 : PAD + at + 1 + PIECE]
    return middle + left + right


def beside(main, other):
    done = 0
    for n, step in enumerate(main):
        step()
        until = len(other) * (n + 1) // len(main)
        for extra in other[done:until]:
            extra()
        done = until


def run(steps):
    for step in steps:
        step()


def fetch_weights(weight_hbm, weight_ref, arrived):
    copies = [
        [pltpu.make_async_copy(weight_hbm.at[i, j], weight_ref.at[i, j], arrived.at[i, j]) for j in range(3)]
        for i in range(3)
    ]
    for part in copies:
        for copy in part:
            copy.start()

    def ready(i):
        for copy in copies[i]:
            copy.wait()

    return ready


def first_kernel(
    prior_ref, inter_ref, intra_ref, gathered_ref, gain_ref, shift_ref, latents_hbm, weight_hbm,
    hidden_ref, totals_ref, *scratch, count,
):
    acts, sums, (weight_ref, arrived, own_ref, own_arrived) = scratch[:4], scratch[4:6], scratch[6:]
    width, channels = own_ref.shape[2], own_ref.shape[3]
    ready = fetch_weights(weight_hbm, weight_ref, arrived)
    fetch_own = pltpu.make_async_copy(latents_hbm, own_ref, own_arrived)
    fetch_own.start()
    for ref in sums:
        clear_pads(ref)
    scale, offset = merge_moments(gathered_ref[...], count, gain_ref[...], shift_ref[...], channels)
    place = position()
    sources = (own_ref, prior_ref, inter_ref, intra_ref)
    acting = [act_steps(f, acts[f], sources, place, scale, offset) for f in range(4)]
    totals = {}

    def finish(t, r, at):
        piece = piece_of(sums[t], r, at)
        hidden_ref[t, r, at : at + PIECE] = piece.astype(BF16)
        if not totals:
            totals["pivot"] = jnp.sum(piece, axis=0, keepdims=True) * (1.0 / PIECE)
            totals["sum"] = jnp.zeros((8, channels), F32)
            totals["square"] = jnp.zeros((8, channels), F32)
        away = (piece - totals["pivot"]).reshape(PIECE // 8, 8, channels)
        totals["sum"] = totals["sum"] + jnp.sum(away, axis=0)
        totals["square"] = totals["square"] + jnp.sum(away * away, axis=0)

    def finishing(t):
        return [functools.partial(finish, t, r, at) for r in range(2) for at in range(0, width, PIECE)]

    taps = lambda f, t: conv_steps(acts[f], weight_ref, f - t, sums[t])
    run(acting[0] + acting[1])
    ready(0)
    run(taps(0, 0))
    ready(1)
    ready(2)
    fetch_own.wait()
    beside(taps(1, 0) + taps(1, 1), acting[2])
    beside(taps(2, 0) + taps(2, 1), acting[3])
    beside(taps(3, 1), finishing(0))
    run(finishing(1))

    totals_ref[0] = totals["sum"]
    totals_ref[1] = totals["square"]
    totals_ref[2] = jnp.broadcast_to(totals["pivot"], (8, channels))


def pack_kernel(totals_ref, bias_ref, moments_ref, *, cells):
    shape = totals_ref.shape[1:]
    away = jnp.broadcast_to(jnp.sum(totals_ref[0], axis=0, keepdims=True), shape)
    square = jnp.broadcast_to(jnp.sum(totals_ref[1], axis=0, keepdims=True), shape)
    square = jnp.maximum(square - away * away * (1.0 / cells), 0.0)
    total = away + cells * (totals_ref[2] + bias_ref[...])
    moments_ref[...] = jnp.broadcast_to(pack_moments(total, square, cells), moments_ref.shape)


def second_kernel(
    own_ref, prior_ref, inter_ref, intra_ref, gathered_ref, gain_ref, shift_ref, bias1_ref, bias2_ref, up_bias_ref,
    latents_hbm, weight_hbm, up_hbm, video_ref, *scratch, count,
):
    acts, sums = scratch[:4], scratch[4:6]
    wide_ref, block_ref, stage_ref, sent, weight_ref, arrived, latents_ref, up_ref, other_arrived = scratch[6:]
    width, channels = own_ref.shape[2], own_ref.shape[3]
    ready = fetch_weights(weight_hbm, weight_ref, arrived)
    fetch_latents = pltpu.make_async_copy(latents_hbm, latents_ref, other_arrived.at[0])
    fetch_latents.start()
    fetch_up = pltpu.make_async_copy(up_hbm, up_ref, other_arrived.at[1])
    fetch_up.start()
    for ref in sums:
        clear_pads(ref)
    scale, offset = merge_moments(gathered_ref[...], count, gain_ref[...], shift_ref[...], channels)
    offset = offset + bias1_ref[...] * scale
    place = position()
    sources = (own_ref, prior_ref, inter_ref, intra_ref)
    acting = [act_steps(f, acts[f], sources, place, scale, offset) for f in range(4)]

    def sending(t, a, b, r):
        return pltpu.make_async_copy(
            stage_ref.at[t, a, 2 * r + b], video_ref.at[2 * t + a, 2 * r + b], sent.at[t, a, 2 * r + b]
        )

    def finish(t, r, at):
        latents = latents_ref[t, r, at : at + PIECE].astype(F32)
        block = latents + (piece_of(sums[t], r, at) + bias2_ref[...])
        block_ref[t, r * width + at : r * width + at + PIECE] = block.astype(BF16)

    def finishing(t):
        return [functools.partial(finish, t, r, at) for r in range(2) for at in range(0, width, PIECE)]

    def widen(t, a, b, e):
        n = ((2 * a + b) * 2 + e) * channels
        part = jnp.dot(block_ref[t], up_ref[:, n : n + channels], preferred_element_type=F32)
        part = part + up_bias_ref[:, n : n + channels]
        for lane in range(0, channels, LANES):
            wide_ref[2 * a + b, lane // LANES, pl.ds(e, 2 * width, stride=2), :] = part[:, lane : lane + LANES]

    def send(t, a, b):
        for r in range(2):
            for lane in range(0, channels, LANES):
                stage_ref[t, a, 2 * r + b, :, lane : lane + LANES] = wide_ref[
                    2 * a + b, lane // LANES, 2 * width * r : 2 * width * (r + 1), :
                ].astype(BF16)
            sending(t, a, b, r).start()

    def widening(t):
        steps = []
        for a in range(2):
            for b in range(2):
                steps += [functools.partial(widen, t, a, b, e) for e in range(2)]
                steps.append(functools.partial(send, t, a, b))
        return steps

    taps = lambda f, t: conv_steps(acts[f], weight_ref, f - t, sums[t])
    run(acting[0] + acting[1])
    ready(0)
    beside(taps(0, 0), acting[2])
    ready(1)
    ready(2)
    fetch_latents.wait()
    beside(taps(1, 0) + taps(1, 1), acting[3])
    run(taps(2, 0))
    beside(taps(2, 1), finishing(0))
    fetch_up.wait()
    beside(taps(3, 1), widening(0))
    run(finishing(1))
    run(widening(1))
    for t in range(2):
        for a in range(2):
            for b in range(2):
                for r in range(2):
                    sending(t, a, b, r).wait()


def edges_kernel(own_ref, prior_ref, outward_ref, inward_ref):
    core = lax.axis_index("rows_2")
    for f in range(4):
        source = prior_ref.at[f] if f < 2 else own_ref.at[f - 2]
        outward_ref[f] = source[core]
        inward_ref[f] = source[1 - core]


VMEM = pl.BlockSpec(memory_space=pltpu.MemorySpace.VMEM)
HBM = pl.BlockSpec(memory_space=pltpu.MemorySpace.HBM)


def in_hbm(x):
    return pltpu.with_memory_space_constraint(x, pltpu.MemorySpace.HBM)


def params(mebibytes):
    return pltpu.CompilerParams(
        vmem_limit_bytes=mebibytes * 1024 * 1024
    )


def send_on(cells):
    return lax.ppermute(cells, "tm", [(i, i + 1) for i in range(lax.axis_size("tm") - 1)])


FIRST = ROWS
SECOND = "tm"


def share(moments, axes):
    return lax.all_to_all(moments, axes, split_axis=0, concat_axis=0, tiled=True)


def share_all(moments, count):
    first = share(moments, FIRST)
    merged = pl.pallas_call(
        functools.partial(merge_kernel, count=count),
        in_specs=[VMEM],
        out_specs=VMEM,
        out_shape=jax.ShapeDtypeStruct((lax.axis_size(SECOND), LANES), F32),
        compiler_params=pltpu.CompilerParams(vmem_limit_bytes=1024 * 1024),
    )(first)
    return share(merged, SECOND)


def send_edges(cells, prior):
    frames, _, width, channels = cells.shape
    edge = jax.ShapeDtypeStruct((2 * frames, width, channels), BF16)
    outward, inward = pl.pallas_call(
        edges_kernel,
        in_specs=[VMEM, VMEM],
        out_specs=[VMEM, VMEM],
        out_shape=[edge, edge],
        compiler_params=pltpu.CompilerParams(vmem_limit_bytes=1024 * 1024),
    )(cells, prior)
    rows = lax.axis_size(ROWS)
    between = [(i, i + 1) for i in range(1, rows - 1, 2)] + [(i + 1, i) for i in range(1, rows - 1, 2)]
    within = [(i, i ^ 1) for i in range(rows)]
    inter = lax.ppermute(outward, ROWS, between)
    intra = lax.ppermute(inward, ROWS, within)
    return inter, intra


def body(
    latents,
    norm1_gain,
    norm1_shift,
    conv1_weight,
    conv1_bias,
    norm2_gain,
    norm2_shift,
    conv2_weight,
    conv2_bias,
    up_weight,
    up_bias,
):
    frames, rows, width, channels = latents.shape
    moments_shape = jax.ShapeDtypeStruct((lax.axis_size(FIRST), LANES), F32)
    cells_shape = jax.ShapeDtypeStruct(latents.shape, BF16)
    acts = [pltpu.VMEM((rows + 2, width, channels), BF16)] * (2 * frames)
    sums = [pltpu.VMEM((3, rows, width + 2 * PAD, channels), F32)] * frames
    one_device = frames * rows * width * (channels // GROUPS)
    one_row = one_device * lax.axis_size(FIRST)
    vectors = (norm1_gain, norm1_shift, conv1_bias, norm2_gain, norm2_shift, conv2_bias, up_bias)
    vectors = [v.reshape(1, -1) for v in vectors]

    prior = send_on(latents)
    moments, own, gain1, shift1, bias1, gain2, shift2, bias2, bias_up = pl.pallas_call(
        stats_kernel,
        in_specs=[HBM] * (1 + len(vectors)),
        out_specs=[VMEM] * (2 + len(vectors)),
        out_shape=[moments_shape, cells_shape] + [jax.ShapeDtypeStruct(v.shape, F32) for v in vectors],
        scratch_shapes=[
            pltpu.SemaphoreType.DMA((frames, rows)),
            pltpu.SemaphoreType.DMA((len(vectors),)),
        ],
        compiler_params=pltpu.CompilerParams(vmem_limit_bytes=1024 * 1024),
    )(*map(in_hbm, (latents, *vectors)))
    inter, intra = send_edges(own, prior)
    gathered = share_all(moments, one_device)
    hidden, totals = pl.pallas_call(
        functools.partial(first_kernel, count=one_row),
        in_specs=[VMEM] * 6 + [HBM] * 2,
        out_specs=[VMEM, VMEM],
        out_shape=[cells_shape, jax.ShapeDtypeStruct((3, 8, channels), F32)],
        scratch_shapes=[
            *acts,
            *sums,
            pltpu.VMEM(conv1_weight.shape, BF16),
            pltpu.SemaphoreType.DMA((3, 3)),
            pltpu.VMEM(latents.shape, BF16),
            pltpu.SemaphoreType.DMA(()),
        ],
        compiler_params=params(20),
    )(prior, inter, intra, gathered, gain1, shift1, in_hbm(latents), in_hbm(conv1_weight))

    prior = send_on(hidden)
    moments = pl.pallas_call(
        functools.partial(pack_kernel, cells=float(frames * rows * width)),
        in_specs=[VMEM, VMEM],
        out_specs=VMEM,
        out_shape=moments_shape,
        compiler_params=params(1),
    )(totals, bias1)
    inter, intra = send_edges(hidden, prior)
    gathered = share_all(moments, one_device)
    return pl.pallas_call(
        functools.partial(second_kernel, count=one_row),
        in_specs=[VMEM] * 10 + [HBM] * 3,
        out_specs=HBM,
        out_shape=jax.ShapeDtypeStruct((2 * frames, 2 * rows, 2 * width, channels), BF16),
        scratch_shapes=[
            *acts,
            *sums,
            pltpu.VMEM((4, channels // LANES, 2 * rows * width, LANES), F32),
            pltpu.VMEM((frames, rows * width, channels), BF16),
            pltpu.VMEM((frames, 2, 2 * rows, 2 * width, channels), BF16),
            pltpu.SemaphoreType.DMA((frames, 2, 2 * rows)),
            pltpu.VMEM(conv2_weight.shape, BF16),
            pltpu.SemaphoreType.DMA((3, 3)),
            pltpu.VMEM(latents.shape, BF16),
            pltpu.VMEM(up_weight.shape, BF16),
            pltpu.SemaphoreType.DMA((2,)),
        ],
        compiler_params=params(32),
    )(
        hidden, prior, inter, intra, gathered, gain2, shift2, bias1, bias2, bias_up,
        in_hbm(latents), in_hbm(conv2_weight), in_hbm(up_weight),
    )


def solution(mesh):
    finer = Mesh(
        mesh.devices.reshape(mesh.shape["tm"], 8, 4, 2), ("tm", "rows_0", "rows_1", "rows_2")
    )
    placed = (P("tm", ROWS, None, None), P(), P(), P(), P(), P(), P(), P(), P(), P(), P())
    return jax.shard_map(
        body, mesh=finer, in_specs=placed, out_specs=P("tm", ROWS, None, None), check_vma=False
    )
```

```python
import functools

import jax
import jax.numpy as jnp
from jax import lax
from jax.experimental import pallas as pl
from jax.experimental.pallas import tpu as pltpu
from jax.sharding import Mesh
from jax.sharding import PartitionSpec as P


GROUPS = 32
EPSILON = 1e-06
ROWS = ("rows_0", "rows_1", "rows_2")
F32 = jnp.float32
BF16 = jnp.bfloat16
LANES = 128


def split_rows(first, second):
    row = lax.broadcasted_iota(jnp.int32, first.shape, 0)
    value = jnp.where(row < 3, first, second)
    high = value.astype(BF16).astype(F32)
    middle = (value - high).astype(BF16).astype(F32)
    low = value - high - middle
    step = jnp.where(row < 3, row, row - 3)
    part = jnp.where(step == 0, high, jnp.where(step == 1, middle, low))
    return jnp.where(row < 6, part, 0.0).astype(BF16)


def joined_rows(product):
    row = lax.broadcasted_iota(jnp.int32, product.shape, 0)
    first = jnp.sum(jnp.where(row < 3, product, 0.0), axis=0, keepdims=True)
    second = jnp.sum(jnp.where((row >= 3) & (row < 6), product, 0.0), axis=0, keepdims=True)
    return first, second


def group_sum(value, per_group):
    lane = lax.broadcasted_iota(jnp.int32, value.shape, 1)
    channels = value.shape[1]
    step = 1
    while step < per_group:
        other = jnp.where(lane & step == 0, pltpu.roll(value, channels - step, 1), pltpu.roll(value, step, 1))
        value = value + other
        step *= 2
    return value


def pack_moments(channel_sum, channel_square, count):
    channels = channel_sum.shape[1]
    per_group = channels // GROUPS
    channel_mean = channel_sum * (1.0 / count)
    group_mean = group_sum(channel_mean, per_group) * (1.0 / per_group)
    spread = channel_mean - group_mean
    square = channel_square + spread * spread * count
    lane = lax.broadcasted_iota(jnp.int32, (channels, LANES), 1)
    group = lax.broadcasted_iota(jnp.int32, (channels, LANES), 0) // per_group
    chosen = ((lane == group) | (lane == group + GROUPS)).astype(F32).astype(BF16)
    product = jnp.dot(split_rows(channel_mean * (1.0 / per_group), square), chosen, preferred_element_type=F32)
    mean, square = joined_rows(product)
    lane = lax.broadcasted_iota(jnp.int32, (1, LANES), 1)
    return jnp.where(lane < GROUPS, mean, square)


def merge_moments(gathered, count, gain, shift, channels):
    devices = gathered.shape[0]
    per_group = channels // GROUPS
    total = jnp.broadcast_to(jnp.sum(gathered, axis=0, keepdims=True), (8, LANES))
    away = gathered - (total * (1.0 / devices))[0:1]
    between = jnp.broadcast_to(jnp.sum(away * away, axis=0, keepdims=True), (8, LANES))
    lane = lax.broadcasted_iota(jnp.int32, (LANES, 2 * channels), 0)
    column = lax.broadcasted_iota(jnp.int32, (LANES, 2 * channels), 1)
    chosen = (lane == column // per_group).astype(F32).astype(BF16)
    product = jnp.dot(split_rows(total, between), chosen, preferred_element_type=F32)
    first, second = joined_rows(product)
    mean = first[:, :channels] * (1.0 / devices)
    within = first[:, channels:]
    variance = (within + second[:, :channels] * count) * (1.0 / (count * devices))
    scale = gain / jnp.sqrt(variance + EPSILON)
    return 0.5 * scale, 0.5 * (shift - mean * scale)


def merge_kernel(gathered_ref, out_ref, *, count):
    gathered = gathered_ref[...]
    members = gathered.shape[0]
    total = jnp.sum(gathered, axis=0, keepdims=True)
    mean = total * (1.0 / members)
    away = gathered - mean
    between = jnp.broadcast_to(jnp.sum(away * away, axis=0, keepdims=True), (8, LANES))
    square = total + pltpu.roll(between, GROUPS, 1)[0:1] * count
    lane = lax.broadcasted_iota(jnp.int32, (1, LANES), 1)
    out_ref[...] = jnp.broadcast_to(jnp.where(lane < GROUPS, mean, square), out_ref.shape)


def stats_kernel(values_ref, *refs):
    fetched = (len(refs) - 4) // 2
    sources = refs[:fetched]
    out_ref, own_ref = refs[fetched : fetched + 2]
    targets = refs[fetched + 2 : 2 * fetched + 2]
    arrived, vectors_arrived = refs[2 * fetched + 2 :]
    frames, rows, width, channels = own_ref.shape
    count = frames * rows * width
    copies = [
        [pltpu.make_async_copy(values_ref.at[f, r], own_ref.at[f, r], arrived.at[f, r]) for r in range(rows)]
        for f in range(frames)
    ]
    for f in range(frames):
        for r in range(rows):
            copies[f][r].start()
    fetches = [pltpu.make_async_copy(sources[i], targets[i], vectors_arrived.at[i]) for i in range(fetched)]
    for fetch in fetches:
        fetch.start()
    acc = jnp.zeros((8, channels), F32)
    for f in range(frames):
        for r in range(rows):
            copies[f][r].wait()
            acc = acc + jnp.sum(own_ref[f, r].astype(F32).reshape(width // 8, 8, channels), axis=0)
    channel_sum = jnp.broadcast_to(jnp.sum(acc, axis=0, keepdims=True), (8, channels))
    mean = channel_sum * (1.0 / count)
    acc = jnp.zeros((8, channels), F32)
    for f in range(frames):
        for r in range(rows):
            away = own_ref[f, r].astype(F32).reshape(width // 8, 8, channels) - mean[None]
            acc = acc + jnp.sum(away * away, axis=0)
    channel_square = jnp.broadcast_to(jnp.sum(acc, axis=0, keepdims=True), (8, channels))
    packed = pack_moments(channel_sum, channel_square, count)
    out_ref[...] = jnp.broadcast_to(packed, out_ref.shape)
    for fetch in fetches:
        fetch.wait()


PIECE = 64
PAD = 8


def position():
    core = lax.axis_index("rows_2")
    row_block = lax.axis_index(ROWS)
    last = lax.axis_size(ROWS) - 1
    inter_exists = jnp.where(core == 0, row_block > 0, row_block < last)
    frames_exist = lax.axis_index("tm") > 0
    return core, jnp.where(frames_exist, 1.0, 0.0).astype(F32), jnp.where(inter_exists, 1.0, 0.0).astype(F32)


def act_steps(f, act_ref, sources, place, scale, offset):
    own_ref, prior_ref, inter_ref, intra_ref = sources
    core, frames_exist, inter_exists = place
    width = own_ref.shape[2]
    half = PIECE // 2
    source = prior_ref.at[f] if f < 2 else own_ref.at[f - 2]
    keep = frames_exist if f < 2 else None
    inter_keep = inter_exists if keep is None else keep * inter_exists
    blocks = [
        (inter_ref.at[f], core * 3, inter_keep),
        (source.at[0], 1, keep),
        (source.at[1], 2, keep),
        (intra_ref.at[f], 3 - core * 3, keep),
    ]

    def step(block, at):
        cells, row, keep = block
        v = cells[at : at + half].astype(F32)
        h = v * scale + offset
        silu = h + h * jnp.tanh(h)
        if keep is not None:
            silu = silu * keep
        act_ref[row, at : at + half] = silu.astype(BF16)

    return [functools.partial(step, block, at) for block in blocks for at in range(0, width, half)]


def conv_steps(act_ref, weight_ref, i, sums_ref):
    width, channels = act_ref.shape[1], act_ref.shape[2]

    def step(k):
        part = None
        for j in range(3):
            window = act_ref[j : j + 2].reshape(2 * width, channels)
            product = jnp.dot(window, weight_ref[i, j, k], preferred_element_type=F32)
            part = product if part is None else part + product
        for r in range(2):
            row = part[r * width : (r + 1) * width]
            if i > 0:
                row = row + sums_ref[k, r, PAD : PAD + width]
            sums_ref[k, r, PAD : PAD + width] = row

    return [functools.partial(step, k) for k in range(3)]


def clear_pads(sums_ref):
    width = sums_ref.shape[2] - 2 * PAD
    channels = sums_ref.shape[3]
    for r in range(2):
        sums_ref[0, r, 0:PAD] = jnp.zeros((PAD, channels), F32)
        sums_ref[2, r, PAD + width :] = jnp.zeros((PAD, channels), F32)


def piece_of(sums_ref, r, at):
    left = sums_ref[0, r, PAD + at - 1 : PAD + at - 1 + PIECE]
    middle = sums_ref[1, r, PAD + at : PAD + at + PIECE]
    right = sums_ref[2, r, PAD + at + 1 : PAD + at + 1 + PIECE]
    return middle + left + right


def beside(main, other):
    done = 0
    for n, step in enumerate(main):
        step()
        until = len(other) * (n + 1) // len(main)
        for extra in other[done:until]:
            extra()
        done = until


def run(steps):
    for step in steps:
        step()


def fetch_weights(weight_hbm, weight_ref, arrived, after_first=None):
    copies = [
        [pltpu.make_async_copy(weight_hbm.at[i, j], weight_ref.at[i, j], arrived.at[i, j]) for j in range(3)]
        for i in range(3)
    ]
    for i, part in enumerate(copies):
        for copy in part:
            copy.start()
        if i == 0 and after_first is not None:
            after_first.start()

    def ready(i):
        for copy in copies[i]:
            copy.wait()

    return ready


def first_kernel(
    prior_ref, inter_ref, intra_ref, gathered_ref, gain_ref, shift_ref, latents_hbm, weight_hbm,
    hidden_ref, totals_ref, *scratch, count,
):
    acts, sums, (weight_ref, arrived, own_ref, own_arrived) = scratch[:4], scratch[4:6], scratch[6:]
    width, channels = own_ref.shape[2], own_ref.shape[3]
    fetch_own = pltpu.make_async_copy(latents_hbm, own_ref, own_arrived)
    ready = fetch_weights(weight_hbm, weight_ref, arrived, fetch_own)
    for ref in sums:
        clear_pads(ref)
    scale, offset = merge_moments(gathered_ref[...], count, gain_ref[...], shift_ref[...], channels)
    place = position()
    sources = (own_ref, prior_ref, inter_ref, intra_ref)
    acting = [act_steps(f, acts[f], sources, place, scale, offset) for f in range(4)]
    totals = {}

    def finish(t, r, at):
        piece = piece_of(sums[t], r, at)
        hidden_ref[t, r, at : at + PIECE] = piece.astype(BF16)
        if not totals:
            totals["pivot"] = jnp.sum(piece, axis=0, keepdims=True) * (1.0 / PIECE)
            totals["sum"] = jnp.zeros((8, channels), F32)
            totals["square"] = jnp.zeros((8, channels), F32)
        away = (piece - totals["pivot"]).reshape(PIECE // 8, 8, channels)
        totals["sum"] = totals["sum"] + jnp.sum(away, axis=0)
        totals["square"] = totals["square"] + jnp.sum(away * away, axis=0)

    def finishing(t):
        return [functools.partial(finish, t, r, at) for r in range(2) for at in range(0, width, PIECE)]

    taps = lambda f, t: conv_steps(acts[f], weight_ref, f - t, sums[t])
    run(acting[0] + acting[1])
    ready(0)
    run(taps(0, 0))
    ready(1)
    fetch_own.wait()
    beside(taps(1, 1) + taps(1, 0), acting[2])
    ready(2)
    beside(taps(2, 0) + taps(2, 1), acting[3])
    beside(taps(3, 1), finishing(0))
    run(finishing(1))

    totals_ref[0] = totals["sum"]
    totals_ref[1] = totals["square"]
    totals_ref[2] = jnp.broadcast_to(totals["pivot"], (8, channels))


def pack_kernel(totals_ref, bias_ref, moments_ref, *, cells):
    shape = totals_ref.shape[1:]
    away = jnp.broadcast_to(jnp.sum(totals_ref[0], axis=0, keepdims=True), shape)
    square = jnp.broadcast_to(jnp.sum(totals_ref[1], axis=0, keepdims=True), shape)
    square = jnp.maximum(square - away * away * (1.0 / cells), 0.0)
    total = away + cells * (totals_ref[2] + bias_ref[...])
    moments_ref[...] = jnp.broadcast_to(pack_moments(total, square, cells), moments_ref.shape)


def second_kernel(
    own_ref, prior_ref, inter_ref, intra_ref, gathered_ref, gain_ref, shift_ref, bias1_ref, bias2_ref, up_bias_ref,
    latents_hbm, weight_hbm, up_hbm, video_ref, *scratch, count,
):
    acts, sums = scratch[:4], scratch[4:6]
    wide_ref, block_ref, stage_ref, sent, weight_ref, arrived, latents_ref, up_ref, other_arrived = scratch[6:]
    width, channels = own_ref.shape[2], own_ref.shape[3]
    ready = fetch_weights(weight_hbm, weight_ref, arrived)
    fetch_latents = pltpu.make_async_copy(latents_hbm, latents_ref, other_arrived.at[0])
    fetch_latents.start()
    fetch_up = pltpu.make_async_copy(up_hbm, up_ref, other_arrived.at[1])
    fetch_up.start()
    for ref in sums:
        clear_pads(ref)
    scale, offset = merge_moments(gathered_ref[...], count, gain_ref[...], shift_ref[...], channels)
    offset = offset + bias1_ref[...] * scale
    place = position()
    sources = (own_ref, prior_ref, inter_ref, intra_ref)
    acting = [act_steps(f, acts[f], sources, place, scale, offset) for f in range(4)]

    def sending(t, a, b, r):
        return pltpu.make_async_copy(
            stage_ref.at[t, a, 2 * r + b], video_ref.at[2 * t + a, 2 * r + b], sent.at[t, a, 2 * r + b]
        )

    def finish(t, r, at):
        latents = latents_ref[t, r, at : at + PIECE].astype(F32)
        block = latents + (piece_of(sums[t], r, at) + bias2_ref[...])
        block_ref[t, r * width + at : r * width + at + PIECE] = block.astype(BF16)

    def finishing(t):
        return [functools.partial(finish, t, r, at) for r in range(2) for at in range(0, width, PIECE)]

    def widen(t, a, b, e):
        n = ((2 * a + b) * 2 + e) * channels
        part = jnp.dot(block_ref[t], up_ref[:, n : n + channels], preferred_element_type=F32)
        part = part + up_bias_ref[:, n : n + channels]
        for lane in range(0, channels, LANES):
            wide_ref[2 * a + b, lane // LANES, pl.ds(e, 2 * width, stride=2), :] = part[:, lane : lane + LANES]

    def send(t, a, b):
        for r in range(2):
            for lane in range(0, channels, LANES):
                stage_ref[t, a, 2 * r + b, :, lane : lane + LANES] = wide_ref[
                    2 * a + b, lane // LANES, 2 * width * r : 2 * width * (r + 1), :
                ].astype(BF16)
            sending(t, a, b, r).start()

    def widening(t):
        steps = []
        for a in range(2):
            for b in range(2):
                steps += [functools.partial(widen, t, a, b, e) for e in range(2)]
                steps.append(functools.partial(send, t, a, b))
        return steps

    taps = lambda f, t: conv_steps(acts[f], weight_ref, f - t, sums[t])
    run(acting[0] + acting[1])
    ready(0)
    beside(taps(0, 0), acting[2])
    ready(1)
    beside(taps(1, 1) + taps(1, 0), acting[3])
    ready(2)
    fetch_latents.wait()
    run(taps(2, 0))
    beside(taps(2, 1), finishing(0))
    fetch_up.wait()
    beside(taps(3, 1), widening(0))
    run(finishing(1))
    run(widening(1))
    for t in range(2):
        for a in range(2):
            for b in range(2):
                for r in range(2):
                    sending(t, a, b, r).wait()


def edges_kernel(own_ref, prior_ref, outward_ref, inward_ref):
    core = lax.axis_index("rows_2")
    for f in range(4):
        source = prior_ref.at[f] if f < 2 else own_ref.at[f - 2]
        outward_ref[f] = source[core]
        inward_ref[f] = source[1 - core]


VMEM = pl.BlockSpec(memory_space=pltpu.MemorySpace.VMEM)
HBM = pl.BlockSpec(memory_space=pltpu.MemorySpace.HBM)


def in_hbm(x):
    return pltpu.with_memory_space_constraint(x, pltpu.MemorySpace.HBM)


def params(mebibytes):
    return pltpu.CompilerParams(
        vmem_limit_bytes=mebibytes * 1024 * 1024
    )


def send_on(cells):
    return lax.ppermute(cells, "tm", [(i, i + 1) for i in range(lax.axis_size("tm") - 1)])


FIRST = ("rows_0", "rows_1")
SECOND = ("tm", "rows_2")


def share(moments, axes):
    return lax.all_to_all(moments, axes, split_axis=0, concat_axis=0, tiled=True)


def share_all(moments, count):
    first = share(moments, FIRST)
    merged = pl.pallas_call(
        functools.partial(merge_kernel, count=count),
        in_specs=[VMEM],
        out_specs=VMEM,
        out_shape=jax.ShapeDtypeStruct((lax.axis_size(SECOND), LANES), F32),
        compiler_params=pltpu.CompilerParams(vmem_limit_bytes=1024 * 1024),
    )(first)
    return share(merged, SECOND)


def send_edges(cells, prior):
    frames, _, width, channels = cells.shape
    edge = jax.ShapeDtypeStruct((2 * frames, width, channels), BF16)
    outward, inward = pl.pallas_call(
        edges_kernel,
        in_specs=[VMEM, VMEM],
        out_specs=[VMEM, VMEM],
        out_shape=[edge, edge],
        compiler_params=pltpu.CompilerParams(vmem_limit_bytes=1024 * 1024),
    )(cells, prior)
    rows = lax.axis_size(ROWS)
    between = [(i, i + 1) for i in range(1, rows - 1, 2)] + [(i + 1, i) for i in range(1, rows - 1, 2)]
    within = [(i, i ^ 1) for i in range(rows)]
    inter = lax.ppermute(outward, ROWS, between)
    intra = lax.ppermute(inward, ROWS, within)
    return inter, intra


def body(
    latents,
    norm1_gain,
    norm1_shift,
    conv1_weight,
    conv1_bias,
    norm2_gain,
    norm2_shift,
    conv2_weight,
    conv2_bias,
    up_weight,
    up_bias,
):
    frames, rows, width, channels = latents.shape
    moments_shape = jax.ShapeDtypeStruct((lax.axis_size(FIRST), LANES), F32)
    cells_shape = jax.ShapeDtypeStruct(latents.shape, BF16)
    acts = [pltpu.VMEM((rows + 2, width, channels), BF16)] * (2 * frames)
    sums = [pltpu.VMEM((3, rows, width + 2 * PAD, channels), F32)] * frames
    one_device = frames * rows * width * (channels // GROUPS)
    one_row = one_device * lax.axis_size(FIRST)
    vectors = (norm1_gain, norm1_shift, conv1_bias, norm2_gain, norm2_shift, conv2_bias, up_bias)
    vectors = [v.reshape(1, -1) for v in vectors]

    prior = send_on(latents)
    moments, own, gain1, shift1, bias1, gain2, shift2, bias2, bias_up = pl.pallas_call(
        stats_kernel,
        in_specs=[HBM] * (1 + len(vectors)),
        out_specs=[VMEM] * (2 + len(vectors)),
        out_shape=[moments_shape, cells_shape] + [jax.ShapeDtypeStruct(v.shape, F32) for v in vectors],
        scratch_shapes=[
            pltpu.SemaphoreType.DMA((frames, rows)),
            pltpu.SemaphoreType.DMA((len(vectors),)),
        ],
        compiler_params=pltpu.CompilerParams(vmem_limit_bytes=1024 * 1024),
    )(*map(in_hbm, (latents, *vectors)))
    inter, intra = send_edges(own, prior)
    gathered = share_all(moments, one_device)
    hidden, totals = pl.pallas_call(
        functools.partial(first_kernel, count=one_row),
        in_specs=[VMEM] * 6 + [HBM] * 2,
        out_specs=[VMEM, VMEM],
        out_shape=[cells_shape, jax.ShapeDtypeStruct((3, 8, channels), F32)],
        scratch_shapes=[
            *acts,
            *sums,
            pltpu.VMEM(conv1_weight.shape, BF16),
            pltpu.SemaphoreType.DMA((3, 3)),
            pltpu.VMEM(latents.shape, BF16),
            pltpu.SemaphoreType.DMA(()),
        ],
        compiler_params=params(20),
    )(prior, inter, intra, gathered, gain1, shift1, in_hbm(latents), in_hbm(conv1_weight))

    prior = send_on(hidden)
    moments = pl.pallas_call(
        functools.partial(pack_kernel, cells=float(frames * rows * width)),
        in_specs=[VMEM, VMEM],
        out_specs=VMEM,
        out_shape=moments_shape,
        compiler_params=params(1),
    )(totals, bias1)
    inter, intra = send_edges(hidden, prior)
    gathered = share_all(moments, one_device)
    return pl.pallas_call(
        functools.partial(second_kernel, count=one_row),
        in_specs=[VMEM] * 10 + [HBM] * 3,
        out_specs=HBM,
        out_shape=jax.ShapeDtypeStruct((2 * frames, 2 * rows, 2 * width, channels), BF16),
        scratch_shapes=[
            *acts,
            *sums,
            pltpu.VMEM((4, channels // LANES, 2 * rows * width, LANES), F32),
            pltpu.VMEM((frames, rows * width, channels), BF16),
            pltpu.VMEM((frames, 2, 2 * rows, 2 * width, channels), BF16),
            pltpu.SemaphoreType.DMA((frames, 2, 2 * rows)),
            pltpu.VMEM(conv2_weight.shape, BF16),
            pltpu.SemaphoreType.DMA((3, 3)),
            pltpu.VMEM(latents.shape, BF16),
            pltpu.VMEM(up_weight.shape, BF16),
            pltpu.SemaphoreType.DMA((2,)),
        ],
        compiler_params=params(32),
    )(
        hidden, prior, inter, intra, gathered, gain2, shift2, bias1, bias2, bias_up,
        in_hbm(latents), in_hbm(conv2_weight), in_hbm(up_weight),
    )


def solution(mesh):
    finer = Mesh(
        mesh.devices.reshape(mesh.shape["tm"], 8, 4, 2), ("tm", "rows_0", "rows_1", "rows_2")
    )
    placed = (P("tm", ROWS, None, None), P(), P(), P(), P(), P(), P(), P(), P(), P(), P())
    return jax.shard_map(
        body, mesh=finer, in_specs=placed, out_specs=P("tm", ROWS, None, None), check_vma=False
    )
```
